256 devices in a mesh: section: 8 (over z), ex: 4 (over x), ey: 8 (over y, core).
Axes of the slice: x: 4, y: 4, z: 8, core: 2. Of those that a mesh axis runs over, the one named last changes fastest.
Arguments:
- section_out: bfloat16 [8, 2048, 7168], P('section', ('ex', 'ey')), may hold values from -6 to 6
- expert_ids: int32 [8, 2048, 2], P('section', ('ex', 'ey')), may hold values from 0 to 7, all different within a row; in each aligned block of 64 rows (0 to 63, 64 to 127, ..., all dimensions but the last counted through in order) at most 24 rows name the same one
- gate_weights: float32 [8, 2048, 2], P('section', ('ex', 'ey')), may hold values from 0.1 to 1
- w_gate_up: bfloat16 [8, 8, 7168, 2, 1024], P('section', 'ey', None, None, 'ex'), may hold values from -0.0625 to 0.0625
- w_down: bfloat16 [8, 8, 1024, 7168], P('section', 'ey', 'ex'), may hold values from -0.1875 to 0.1875
Outputs:
- next_state: bfloat16 [8, 2048, 7168], P('section', ('ex', 'ey'))
The draws below stay inside these ranges and needn't reach their ends.
Inputs may be any that keep to these rules, and one draw needn't show every extreme that they name: `expert_ids`: each row names 2 different experts. In the rows of one device (aligned blocks of 64 rows, all leading dimensions in order) no expert is named by more than 24 rows, and some block of every draw names one expert exactly 24 times.
All inputs are finite; a program needn't handle non-finite values.
Results may differ from the reference program's by a relative error of at most 0.008.
Values may be sent and summed in bfloat16 or wider, within the bound.
A program may use at most 128 MiB of HBM per device.

```python
import math
import jax
import jax.numpy as jnp
import numpy as np
from jax import lax

D = 7168
FF = 1024
TOP = 2
TOK_DEV = 64
SECTIONS = 8
EXPERTS = 8
TOKENS = 2048
CAP = 24
N_EX = 4


def level_of(key, extent, shards, smallest, high):
    loudness, own = 1.0, jax.random.fold_in(key, 6)
    for dim, blocks in shards:
        heights = jnp.exp(jax.random.uniform(jax.random.fold_in(own, dim), (blocks,), jnp.float32, smallest / len(shards), high / len(shards)))
        loudness = loudness * jnp.repeat(heights, extent[dim] // blocks).reshape([-1 if axis == dim else 1 for axis in range(len(extent))])
    return loudness


def shared_out(rng, own, number, rows, number_of, top, reach, slope):
    ranking = jax.random.permutation(rng, number_of)
    crowded, usual = shares(number_of, rows * top, reach, slope, True), shares(number_of, rows * top, reach, slope, False)
    places = jnp.arange(number_of)

    def named(tallies, rotation):
        used = int((tallies > 0).sum())
        fixed = max(1, used // 4)
        shifted = fixed + (places - fixed + rotation * (used - fixed)) % max(1, number_of - fixed)
        return jnp.zeros((number_of,), jnp.int32).at[ranking[jnp.where(places < fixed, places, shifted)]].set(jnp.asarray(tallies, jnp.int32))

    tallies = jnp.where(number % 4 == 0, named(crowded, number // 4), named(usual, number - number // 4 - 1))
    mixed = jax.random.permutation(jax.random.fold_in(own, 3), number_of)
    donor, taker = mixed[0:number_of // 2 * 2:2], mixed[1:number_of // 2 * 2:2]
    room = jnp.minimum(tallies[donor] - 1, reach - tallies[taker]) // 2
    room = jnp.where((donor == ranking[0]) | (taker == ranking[0]) | (tallies[taker] == 0), 0, jnp.maximum(room, 0))
    shifted = jax.random.randint(jax.random.fold_in(own, 4), (number_of // 2,), 0, 1 << 20) % (room + 1)
    tallies = tallies.at[donor].add(-shifted).at[taker].add(shifted)
    items = jnp.searchsorted(jnp.cumsum(tallies), jnp.arange(rows * top), side="right").astype(jnp.int32)
    table = items.reshape(top, rows).T
    table = table[jax.random.permutation(jax.random.fold_in(own, 1), rows)]
    rotation = jax.random.randint(jax.random.fold_in(own, 2), (rows, 1), 0, top)
    return jnp.take_along_axis(table, (jnp.arange(top)[None, :] + rotation) % top, axis=1)


def shares(amount, total, bound, skew, full):
    loads = [(1 << 20) // math.isqrt(standing ** skew) + 1 for standing in range(1, amount + 1)]
    largest = bound if full else min(bound, max(-(-total // amount), total * loads[0] // sum(loads)))
    least = 1 if total - largest >= amount - 1 else 0
    given, spare = [largest] + [least] * (amount - 1), total - largest - least * (amount - 1)
    while spare > 0:
        movable = [i for i in range(1, amount) if given[i] < largest] or [i for i in range(1, amount) if given[i] < bound]
        pool, left = sum([loads[i] for i in movable]), spare
        for i in movable:
            more = min(bound - given[i], max(1, left * loads[i] // pool), spare)
            given[i] = given[i] + more
            spare = spare - more
    return np.array(given)


def centred(key, extent, scale, limit, split=(), held_as=jnp.bfloat16):
    array = scale * jax.random.normal(key, extent, jnp.float32)
    if split:
        array = array * level_of(key, extent, split, -0.22, 0.18)
    return jnp.clip(array, -limit, limit).astype(held_as)


def setup_inputs(seed: int = 0) -> dict:
    key_list = jax.random.split(jax.random.key(seed), 6)
    section_out = centred(key_list[0], (SECTIONS, TOKENS, D), 1.0, 6.0, ((0, 8), (1, 32)))
    expert_ids_keys = jax.random.split(jax.random.fold_in(key_list[1], 1), SECTIONS * TOKENS // TOK_DEV)
    expert_ids_turns = jax.random.permutation(jax.random.fold_in(key_list[1], 3), SECTIONS * TOKENS // TOK_DEV)
    expert_ids = jax.vmap(lambda own, number: shared_out(jax.random.fold_in(key_list[1], 2), own, number, TOK_DEV, EXPERTS, TOP, CAP, 2))(expert_ids_keys, expert_ids_turns).reshape((SECTIONS, TOKENS, TOP))
    gate_weights = jnp.clip(jnp.exp(math.log(1.0) - 2.3025851 * jax.random.uniform(key_list[2], (SECTIONS, TOKENS, TOP), jnp.float32) ** level_of(key_list[2], (SECTIONS, TOKENS, TOP), ((0, 8), (1, 32)), -0.2, 0.2)), 0.1, 1.0)
    w_gate_up = centred(key_list[3], (SECTIONS, EXPERTS, D, 2, FF), D ** -0.5, 0.0625, ((0, 8), (1, 8), (4, 4)))
    w_down = centred(key_list[4], (SECTIONS, EXPERTS, FF, D), FF ** -0.5, 0.1875, ((0, 8), (1, 8), (2, 4)))
    return dict(section_out=section_out, expert_ids=expert_ids, gate_weights=gate_weights, w_gate_up=w_gate_up, w_down=w_down)


def route_section(section_args):
    incoming, chosen_ids, gates, gate_up, down_proj = section_args
    devices = TOKENS // TOK_DEV
    slot_total = devices * CAP
    flat_ids = chosen_ids.reshape(devices, TOK_DEV * TOP)
    one_hot = (flat_ids[:, :, None] == jnp.arange(EXPERTS, dtype=jnp.int32)[None, None, :]).astype(jnp.int32)
    slot_rank = jnp.sum((jnp.cumsum(one_hot, axis=1) - one_hot) * one_hot, axis=2)
    device_ids = jnp.arange(devices, dtype=jnp.int32)[:, None]
    position = (flat_ids * slot_total + device_ids * CAP + slot_rank).reshape(-1).astype(jnp.int32)
    token_of = jnp.arange(TOKENS * TOP, dtype=jnp.int32) // TOP
    source_row = jnp.zeros((EXPERTS * slot_total,), jnp.int32).at[position].set(token_of)
    slice_width = FF // N_EX

    def one_expert(expert_args):
        expert_index, weight_rows, down_rows = expert_args
        chosen_rows = lax.dynamic_slice_in_dim(source_row, expert_index * slot_total, slot_total)
        token_rows = incoming[chosen_rows]
        mixed = jnp.dot(token_rows, weight_rows.reshape(D, 2 * FF), preferred_element_type=jnp.float32)
        hidden = (jax.nn.silu(mixed[:, :FF]) * mixed[:, FF:]).astype(jnp.bfloat16)
        slice_parts = jnp.einsum("rqf,qfd->qrd", hidden.reshape(slot_total, N_EX, slice_width).astype(jnp.float32),
                                 down_rows.reshape(N_EX, slice_width, D).astype(jnp.float32))
        rounded = lax.optimization_barrier(slice_parts.astype(jnp.bfloat16))
        return jnp.sum(rounded.astype(jnp.float32), axis=0).astype(jnp.bfloat16)

    expert_out = lax.map(one_expert, (jnp.arange(EXPERTS, dtype=jnp.int32), gate_up, down_proj))
    picked = expert_out.reshape(EXPERTS * slot_total, D)[position].reshape(TOKENS, TOP, D)
    weighted = jnp.einsum("tkd,tk->td", picked.astype(jnp.float32), gates.astype(jnp.float32))
    return (incoming.astype(jnp.float32) + weighted).astype(jnp.bfloat16)


def reference(section_out, expert_ids, gate_weights, w_gate_up, w_down):
    incoming = jnp.roll(section_out, 1, axis=0)
    return lax.map(route_section, (incoming, expert_ids, gate_weights, w_gate_up, w_down))
```

```python
import jax
import jax.numpy as jnp
from jax import lax
from jax.experimental import pallas as pl
from jax.experimental.pallas import tpu as pltpu
from jax.sharding import PartitionSpec as P

MESH = pl.DeviceIdType.MESH
ROWS = 16
EXT = 128
BF = jnp.bfloat16
F32 = jnp.float32


def moe_kernel(
    sec_ref, gate_ref, wgu_hbm, wd_hbm, out_ref,
    xb, zin, ext, wgu, wd, acc, hid, part, peer, rb, tot, rb2,
    wsem, zsend, zrecv, agr, ags, prd, pds, relay, meet, rsend, relay2, meet2, rsend2, free_x, free_p,
):
    groups = zin.shape[0]
    width = zin.shape[2]
    units = wd.shape[0]
    quarter = width // 4
    half = EXT + 2 * quarter
    whole = EXT + width
    col_a, col_b = pl.ds(0, half), pl.ds(half, 2 * quarter)
    col_q = (
        pl.ds(0, EXT + quarter), pl.ds(EXT + quarter, quarter),
        pl.ds(half, quarter), pl.ds(half + quarter, quarter),
    )
    sec = lax.axis_index("section")
    x = lax.axis_index("ex")
    ey = lax.axis_index("ey")
    y, c = lax.div(ey, 2), lax.rem(ey, 2)
    co = 1 - c
    n_sec = lax.axis_size("section")
    xp, xm, xd = lax.rem(x + 1, 4), lax.rem(x + 3, 4), lax.rem(x + 2, 4)
    yp, ym, yd = lax.rem(y + 1, 4), lax.rem(y + 3, 4), lax.rem(y + 2, 4)
    zp, zm = lax.rem(sec + 1, n_sec), lax.rem(sec + n_sec - 1, n_sec)
    to_xp, to_xm = (sec, xp, ey), (sec, xm, ey)
    to_yp, to_ym = (sec, x, yp * 2 + c), (sec, x, ym * 2 + c)
    to_peer = (sec, x, y * 2 + co)
    to_zp, to_zm = (zp, x, ey), (zm, x, ey)

    def rdma(src, dst, ssem, rsem, device):
        return pltpu.make_async_remote_copy(
            src_ref=src, dst_ref=dst, send_sem=ssem, recv_sem=rsem, device_id=device, device_id_type=MESH
        )

    def wait_recv(ref, sem):
        rdma(ref, ref, sem, sem, to_peer).wait_recv()

    def wait_send(ref, sem):
        rdma(ref, ref, sem, sem, to_peer).wait_send()

    barrier = pltpu.get_barrier_semaphore()
    for device in (to_xp, to_xm, to_yp, to_ym, to_peer, to_zp, to_zm):
        pl.semaphore_signal(barrier, inc=1, device_id=device, device_id_type=MESH)
    pl.semaphore_wait(barrier, 7)

    for g in range(groups):
        rdma(sec_ref.at[pl.ds(g * ROWS, ROWS)], zin.at[g], zsend.at[g], zrecv.at[g], to_zp).start()
    load_gu = pltpu.make_async_copy(wgu_hbm, wgu, wsem.at[0])
    load_d = pltpu.make_async_copy(wd_hbm, wd, wsem.at[1])
    load_gu.start()
    load_d.start()

    gate = gate_ref[...]
    high = gate.astype(BF).astype(F32)
    mid = (gate - high).astype(BF).astype(F32)
    low = gate - high - mid
    lane = lax.broadcasted_iota(jnp.int32, gate.shape, 1)
    ext[...] = jnp.where(lane < 8, high, jnp.where(lane < 16, mid, low)).astype(BF).reshape(ext.shape)

    def gather_1(a, p):
        @pl.when(a >= 2)
        def _():
            pl.semaphore_wait(free_x.at[a - 2], 5)

        wait_recv(zin.at[a], zrecv.at[a])
        own = xb.at[p, c, y, x]
        own[:, pl.ds(0, EXT)] = ext[a]
        own[:, pl.ds(EXT, width)] = zin[a]
        own_a, own_b = own.at[:, col_a], own.at[:, col_b]
        rdma(own_a, own_a, ags.at[a, 0], agr.at[a, 0], to_xp).start()
        rdma(own_a, own_a, ags.at[a, 0], agr.at[a, 1], to_xm).start()
        rdma(own_b, own_b, ags.at[a, 0], agr.at[a, 2], to_yp).start()
        rdma(own_b, own_b, ags.at[a, 0], agr.at[a, 3], to_ym).start()
        rdma(own, own, ags.at[a, 4], agr.at[a, 16], to_peer).start()
        spread(a, p, x, y)

    def spread(a, p, bx, by):
        src_a, src_b = xb.at[p, c, y, bx, :, col_a], xb.at[p, c, by, x, :, col_b]
        rdma(src_a, src_a, ags.at[a, 2], agr.at[a, 8], to_yp).start()
        rdma(src_a, src_a, ags.at[a, 2], agr.at[a, 9], to_ym).start()
        rdma(src_b, src_b, ags.at[a, 2], agr.at[a, 10], to_xp).start()
        rdma(src_b, src_b, ags.at[a, 2], agr.at[a, 11], to_xm).start()

    def to_partner(a, ref):
        rdma(ref, ref, ags.at[a, 4], agr.at[a, 16], to_peer).start()

    def gather_2(a, p):
        left, right = xb.at[p, c, y, xm], xb.at[p, c, y, xp]
        below, above = xb.at[p, c, ym, x], xb.at[p, c, yp, x]
        wait_recv(left.at[:, col_a], agr.at[a, 0])
        rdma(left.at[:, col_q[0]], left.at[:, col_q[0]], ags.at[a, 1], agr.at[a, 4], to_xp).start()
        wait_recv(right.at[:, col_a], agr.at[a, 1])
        rdma(right.at[:, col_q[1]], right.at[:, col_q[1]], ags.at[a, 1], agr.at[a, 5], to_xm).start()
        wait_recv(below.at[:, col_b], agr.at[a, 2])
        rdma(below.at[:, col_q[2]], below.at[:, col_q[2]], ags.at[a, 1], agr.at[a, 6], to_yp).start()
        wait_recv(above.at[:, col_b], agr.at[a, 3])
        rdma(above.at[:, col_q[3]], above.at[:, col_q[3]], ags.at[a, 1], agr.at[a, 7], to_ym).start()
        spread(a, p, xm, ym)
        spread(a, p, xp, yp)
        for ref in (left.at[:, col_a], right.at[:, col_a], below.at[:, col_b], above.at[:, col_b]):
            to_partner(a, ref)

    def gather_3(a, p):
        across, over = xb.at[p, c, y, xd], xb.at[p, c, yd, x]
        wait_recv(across.at[:, col_q[0]], agr.at[a, 4])
        wait_recv(across.at[:, col_q[1]], agr.at[a, 5])
        wait_recv(over.at[:, col_q[2]], agr.at[a, 6])
        wait_recv(over.at[:, col_q[3]], agr.at[a, 7])
        spread(a, p, xd, yd)
        to_partner(a, across.at[:, col_a])
        to_partner(a, over.at[:, col_b])

    def gather_4(a, p):
        below, above = xb.at[p, c, ym], xb.at[p, c, yp]
        left, right = xb.at[p, c, :, xm], xb.at[p, c, :, xp]
        wait_recv(below.at[:, :, col_a], agr.at[a, 8])
        rdma(below.at[:, :, col_q[0]], below.at[:, :, col_q[0]], ags.at[a, 3], agr.at[a, 12], to_yp).start()
        wait_recv(above.at[:, :, col_a], agr.at[a, 9])
        rdma(above.at[:, :, col_q[1]], above.at[:, :, col_q[1]], ags.at[a, 3], agr.at[a, 13], to_ym).start()
        wait_recv(left.at[:, :, col_b], agr.at[a, 10])
        rdma(left.at[:, :, col_q[2]], left.at[:, :, col_q[2]], ags.at[a, 3], agr.at[a, 14], to_xp).start()
        wait_recv(right.at[:, :, col_b], agr.at[a, 11])
        rdma(right.at[:, :, col_q[3]], right.at[:, :, col_q[3]], ags.at[a, 3], agr.at[a, 15], to_xm).start()
        for ref in (below.at[:, :, col_a], above.at[:, :, col_a], left.at[:, :, col_b], right.at[:, :, col_b]):
            to_partner(a, ref)

    def gather_5(a, p):
        over, across = xb.at[p, c, yd], xb.at[p, c, :, xd]
        wait_recv(over.at[:, :, col_q[0]], agr.at[a, 12])
        wait_recv(over.at[:, :, col_q[1]], agr.at[a, 13])
        to_partner(a, over.at[:, :, col_a])
        wait_recv(across.at[:, :, col_q[2]], agr.at[a, 14])
        wait_recv(across.at[:, :, col_q[3]], agr.at[a, 15])
        to_partner(a, across.at[:, :, col_b])

    tokens = acc.shape[0]
    depth = quarter if quarter % 256 else quarter // 2

    def up(g, p):
        wait_recv(xb.at[p, co], agr.at[g, 16])

        def step(k, carry):
            at = pl.multiple_of(k * depth, 128)
            rows = xb[p, :, :, :, :, pl.ds(EXT + at, depth)].reshape(tokens, depth)
            term = jnp.dot(rows, wgu[pl.ds(at, depth), :], preferred_element_type=F32)
            acc[...] = jnp.where(k == 0, term, acc[...] + term)
            return carry

        lax.fori_loop(0, width // depth, step, 0)

        def activate(i, carry):
            fours = 4 * ROWS
            at = pl.multiple_of(i * fours, fours)
            coded = xb[p, lax.div(i, 4), lax.rem(i, 4), :, :, pl.ds(0, EXT)].reshape(fours, EXT).astype(F32)
            lanes = lax.broadcasted_iota(jnp.int32, coded.shape, 1)
            weight = jnp.sum(jnp.where(lax.rem(lanes, 8) == ey, coded, 0.0), axis=1, keepdims=True)
            first = acc[pl.ds(at, fours), pl.ds(0, units)]
            second = acc[pl.ds(at, fours), pl.ds(units, units)]
            value = first / (1.0 + jnp.exp(-first)) * second
            hid[pl.ds(at, fours), :] = (value * weight).astype(BF)
            return carry

        lax.fori_loop(0, tokens // (4 * ROWS), activate, 0)
        wait_send(xb.at[p, c, 0, pl.ds(0, 2)], ags.at[g, 0])
        wait_send(xb.at[p, c, 0, 0], ags.at[g, 1])
        wait_send(xb.at[p, c, pl.ds(0, 2)], ags.at[g, 2])
        wait_send(xb.at[p, c, 0], ags.at[g, 3])
        wait_send(xb.at[p, c], ags.at[g, 4])

        @pl.when(g < 2)
        def _():
            for device in (to_xp, to_xm, to_yp, to_ym, to_peer):
                pl.semaphore_signal(free_x.at[g], inc=1, device_id=device, device_id_type=MESH)

    def cols(q):
        return pl.ds(q * quarter, quarter)

    def pick(q, bx, by):
        return part.at[c, by, :, :, cols(q)] if q < 2 else part.at[c, :, bx, :, cols(q)]

    fwd = ((xp, yp), (xm, ym))
    bwd = ((xm, ym), (xp, yp))
    dev_first = ((to_yp, to_ym), (to_ym, to_yp), (to_xp, to_xm), (to_xm, to_xp))
    dev_second = ((to_xp, to_xm), (to_xm, to_xp), (to_yp, to_ym), (to_ym, to_yp))

    def wait_part(g):
        wait_send(part.at[co], pds.at[g])
        wait_send(part.at[c, pl.ds(0, 3)], rsend.at[g])

    def down(g):
        @pl.when(g >= 1)
        def _():
            wait_part(g - 1)
            pl.semaphore_wait(free_p.at[g - 1], 1)

        tile = 256
        for q in range(4):
            def step(j, carry):
                at = pl.multiple_of(q * quarter + j * tile, 128)
                value = jnp.dot(hid[...], wd[:, pl.ds(at, tile)], preferred_element_type=F32)
                part[:, :, :, :, pl.ds(at, tile)] = value.astype(BF).reshape(2, 4, 4, ROWS, tile)
                return carry

            lax.fori_loop(0, quarter // tile, step, 0)
            rdma(part.at[co, :, :, :, cols(q)], peer.at[:, :, :, cols(q)], pds.at[g], prd.at[g, q], to_peer).start()
        for q in range(4):
            wait_recv(peer.at[:, :, :, cols(q)], prd.at[g, q])

            def add(i, carry):
                iy, ix = lax.div(i, 4), lax.rem(i, 4)
                total = part[c, iy, ix, :, cols(q)].astype(F32) + peer[iy, ix, :, cols(q)].astype(F32)
                part[c, iy, ix, :, cols(q)] = total.astype(BF)
                return carry

            lax.fori_loop(0, 16, add, 0)
            k = q % 2
            rdma(pick(q, xd, yd), rb.at[g, q, 0], rsend.at[g], relay.at[g, q], dev_first[q][0]).start()
            rdma(pick(q, *bwd[k]), rb.at[g, q, 1], rsend.at[g], meet.at[g, q], dev_first[q][1]).start()

        @pl.when(g < groups - 1)
        def _():
            pl.semaphore_signal(free_p.at[g], inc=1, device_id=to_peer, device_id_type=MESH)

    def scatter_2(g):
        for q in range(4):
            wait_recv(rb.at[g, q, 0], relay.at[g, q])
            mine = pick(q, *fwd[q % 2])

            def add(i, carry):
                mine[i] = (mine[i].astype(F32) + rb[g, q, 0, i].astype(F32)).astype(BF)
                return carry

            lax.fori_loop(0, 4, add, 0)
            rdma(mine, rb.at[g, q, 2], rsend.at[g], meet.at[g, q], dev_first[q][0]).start()

    def scatter_3(g):
        for q in range(4):
            wait_recv(rb.at[g, q, pl.ds(1, 2)], meet.at[g, q])
            mine = pick(q, x, y)

            def add(i, carry):
                total = mine[i].astype(F32) + rb[g, q, 1, i].astype(F32) + rb[g, q, 2, i].astype(F32)
                tot[q, i] = total.astype(BF)
                return carry

            lax.fori_loop(0, 4, add, 0)
            k = q % 2
            far, back = (xd, bwd[k][0]) if q < 2 else (yd, bwd[k][1])
            rdma(tot.at[q, far], rb2.at[g, q, 0], rsend2.at[g], relay2.at[g, q], dev_second[q][0]).start()
            rdma(tot.at[q, back], rb2.at[g, q, 1], rsend2.at[g], meet2.at[g, q], dev_second[q][1]).start()

    def scatter_4(g):
        for q in range(4):
            wait_recv(rb2.at[g, q, 0], relay2.at[g, q])
            at = fwd[q % 2][0] if q < 2 else fwd[q % 2][1]
            tot[q, at] = (tot[q, at].astype(F32) + rb2[g, q, 0].astype(F32)).astype(BF)
            rdma(tot.at[q, at], rb2.at[g, q, 2], rsend2.at[g], meet2.at[g, q], dev_second[q][0]).start()

    def scatter_5(g):
        rows = pl.ds(pl.multiple_of(g * ROWS, ROWS), ROWS)
        for q in range(4):
            wait_recv(rb2.at[g, q, pl.ds(1, 2)], meet2.at[g, q])
            at = x if q < 2 else y
            total = tot[q, at].astype(F32) + rb2[g, q, 1].astype(F32) + rb2[g, q, 2].astype(F32)
            out_ref[rows, cols(q)] = (total + zin[g, :, cols(q)].astype(F32)).astype(BF)
        wait_send(tot.at[pl.ds(0, 3)], rsend2.at[g])

    def turn(i, carry):
        a, g, t = i, i - 1, i - 2
        pa, pg = lax.rem(a, 2), lax.rem(i + 1, 2)
        gathers = a < groups
        computes = (g >= 0) & (g < groups)
        ends = t >= 0

        @pl.when(i == 1)
        def _():
            load_gu.wait()
            load_d.wait()

        @pl.when(gathers)
        def _():
            gather_1(a, pa)

        @pl.when(computes)
        def _():
            up(g, pg)

        @pl.when(ends)
        def _():
            scatter_3(t)

        @pl.when(gathers)
        def _():
            gather_2(a, pa)

        @pl.when(computes)
        def _():
            down(g)

        @pl.when(ends)
        def _():
            scatter_4(t)

        @pl.when(gathers)
        def _():
            gather_3(a, pa)

        @pl.when(ends)
        def _():
            scatter_5(t)

        @pl.when(gathers)
        def _():
            gather_4(a, pa)

        @pl.when(computes)
        def _():
            scatter_2(g)

        @pl.when(gathers)
        def _():
            gather_5(a, pa)

        return carry

    lax.fori_loop(0, groups + 2, turn, 0)
    wait_part(groups - 1)
    for g in range(groups):
        wait_send(zin.at[g], zsend.at[g])


def on_device(section_out, expert_ids, gate_weights, w_gate_up, w_down):
    rows, width = section_out.shape[1:]
    units = w_down.shape[2]
    groups = rows // ROWS
    quarter = width // 4
    chosen = expert_ids[0][:, :, None] == jnp.arange(8, dtype=jnp.int32)[None, None, :]
    dense = jnp.sum(jnp.where(chosen, gate_weights[0][:, :, None], 0.0), axis=1)
    gates = jnp.concatenate([dense, dense, dense, jnp.zeros((rows, EXT - 24), F32)], axis=1)
    gate_up = w_gate_up[0, 0].reshape(width, 2 * units)
    hbm = pl.BlockSpec(memory_space=pl.ANY)
    vmem = pl.BlockSpec(memory_space=pltpu.VMEM)
    dma = pltpu.SemaphoreType.DMA
    regular = pltpu.SemaphoreType.REGULAR
    result = pl.pallas_call(
        moe_kernel,
        out_shape=jax.ShapeDtypeStruct((rows, width), BF),
        in_specs=[hbm, vmem, hbm, hbm],
        out_specs=vmem,
        scratch_shapes=[
            pltpu.VMEM((2, 2, 4, 4, ROWS, EXT + width), BF),
            pltpu.VMEM((groups, ROWS, width), BF),
            pltpu.VMEM((groups, ROWS, EXT), BF),
            pltpu.VMEM((width, 2 * units), BF),
            pltpu.VMEM((units, width), BF),
            pltpu.VMEM((32 * ROWS, 2 * units), F32),
            pltpu.VMEM((32 * ROWS, units), BF),
            pltpu.VMEM((2, 4, 4, ROWS, width), BF),
            pltpu.VMEM((4, 4, ROWS, width), BF),
            pltpu.VMEM((groups, 4, 3, 4, ROWS, quarter), BF),
            pltpu.VMEM((4, 4, ROWS, quarter), BF),
            pltpu.VMEM((groups, 4, 3, ROWS, quarter), BF),
            dma((2,)), dma((groups,)), dma((groups,)),
            dma((groups, 17)), dma((groups, 5)),
            dma((groups, 4)), dma((groups,)),
            dma((groups, 4)), dma((groups, 4)), dma((groups,)),
            dma((groups, 4)), dma((groups, 4)), dma((groups,)),
            regular((groups,)), regular((groups,)),
        ],
        compiler_params=pltpu.CompilerParams(
            collective_id=0, has_side_effects=True, vmem_limit_bytes=66_000_000
        ),
        name="moe",
    )(section_out[0], gates, gate_up, w_down[0, 0])
    return result[None]


def solution(mesh):
    return jax.shard_map(
        on_device,
        mesh=mesh,
        in_specs=(
            P("section", ("ex", "ey"), None),
            P("section", ("ex", "ey"), None),
            P("section", ("ex", "ey"), None),
            P("section", "ey", None, None, "ex"),
            P("section", "ey", "ex", None),
        ),
        out_specs=P("section", ("ex", "ey"), None),
        check_vma=False,
    )
```

```python
import jax
import jax.numpy as jnp
from jax import lax
from jax.experimental import pallas as pl
from jax.experimental.pallas import tpu as pltpu
from jax.sharding import PartitionSpec as P

MESH = pl.DeviceIdType.MESH
ROWS = 16
EXT = 128
BF = jnp.bfloat16
F32 = jnp.float32


def moe_kernel(
    sec_ref, id_ref, gate_ref, wgu_hbm, wd_hbm, out_ref,
    xb, zin, ext, raw, wgu, wd, acc, hid, part, peer, rb, tot, rb2,
    wsem, zsend, zrecv, agr, ags, prd, pds, relay, meet, rsend, relay2, meet2, rsend2, free_x, free_p,
):
    groups = zin.shape[0]
    width = zin.shape[2]
    units = wd.shape[0]
    quarter = width // 4
    half = EXT + 2 * quarter
    whole = EXT + width
    col_a, col_b = pl.ds(0, half), pl.ds(half, 2 * quarter)
    col_q = (
        pl.ds(0, EXT + quarter), pl.ds(EXT + quarter, quarter),
        pl.ds(half, quarter), pl.ds(half + quarter, quarter),
    )
    sec = lax.axis_index("section")
    x = lax.axis_index("ex")
    ey = lax.axis_index("ey")
    y, c = lax.div(ey, 2), lax.rem(ey, 2)
    co = 1 - c
    n_sec = lax.axis_size("section")
    xp, xm, xd = lax.rem(x + 1, 4), lax.rem(x + 3, 4), lax.rem(x + 2, 4)
    yp, ym, yd = lax.rem(y + 1, 4), lax.rem(y + 3, 4), lax.rem(y + 2, 4)
    zp, zm = lax.rem(sec + 1, n_sec), lax.rem(sec + n_sec - 1, n_sec)
    to_xp, to_xm = (sec, xp, ey), (sec, xm, ey)
    to_yp, to_ym = (sec, x, yp * 2 + c), (sec, x, ym * 2 + c)
    to_peer = (sec, x, y * 2 + co)
    to_zp, to_zm = (zp, x, ey), (zm, x, ey)

    def rdma(src, dst, ssem, rsem, device):
        return pltpu.make_async_remote_copy(
            src_ref=src, dst_ref=dst, send_sem=ssem, recv_sem=rsem, device_id=device, device_id_type=MESH
        )

    def wait_recv(ref, sem):
        rdma(ref, ref, sem, sem, to_peer).wait_recv()

    def wait_send(ref, sem):
        rdma(ref, ref, sem, sem, to_peer).wait_send()

    barrier = pltpu.get_barrier_semaphore()
    for device in (to_xp, to_xm, to_yp, to_ym, to_peer, to_zp, to_zm):
        pl.semaphore_signal(barrier, inc=1, device_id=device, device_id_type=MESH)
    pl.semaphore_wait(barrier, 7)

    def relay_rows(g):
        rows = pl.ds(pl.multiple_of(g * ROWS, ROWS), ROWS)
        return rdma(sec_ref.at[rows], zin.at[g], zsend.at[g], zrecv.at[g], to_zp)

    relay_rows(0).start()
    pieces, piece = width // raw.shape[1], raw.shape[1]

    def load(k, slot):
        return pltpu.make_async_copy(wgu_hbm.at[pl.ds(k * piece, piece)], raw.at[slot], wsem.at[slot])

    load(0, 0).start()
    load(1, 1).start()
    load_d = pltpu.make_async_copy(wd_hbm, wd, wsem.at[2])
    load_d.start()

    row = lax.broadcasted_iota(jnp.int32, (EXT, EXT), 0)
    table = jnp.zeros((EXT, EXT), F32)
    ids = jnp.concatenate([id_ref[...]] * (EXT // id_ref.shape[1]), axis=1)
    weights = jnp.concatenate([gate_ref[...]] * (EXT // gate_ref.shape[1]), axis=1)
    for k in range(ids.shape[0]):
        table = table + jnp.where(lax.rem(row, 8) == ids[k : k + 1], weights[k : k + 1], 0.0)
    high = table.astype(BF).astype(F32)
    mid = (table - high).astype(BF).astype(F32)
    low = table - high - mid
    terms = jnp.where(row < 8, high, jnp.where(row < 16, mid, jnp.where(row < 24, low, 0.0)))
    ext[...] = terms.T[: groups * ROWS].astype(BF).reshape(ext.shape)

    def unpack(first, count):
        for k in range(first, first + count):
            slot = k % 2
            load(k, slot).wait()

            def step(j, carry):
                at = pl.multiple_of(j * 128, 128)
                to = pl.multiple_of(k * piece + j * 128, 128)
                wgu[pl.ds(to, 128), :] = raw[slot, pl.ds(at, 128)].reshape(128, wgu.shape[1])
                return carry

            lax.fori_loop(0, piece // 128, step, 0)
            if k + 2 < pieces:
                load(k + 2, slot).start()

    def gather_1(a, p):
        @pl.when(a >= 2)
        def _():
            pl.semaphore_wait(free_x.at[a - 2], 5)

        wait_recv(zin.at[a], zrecv.at[a])

        @pl.when(a + 1 < groups)
        def _():
            relay_rows(a + 1).start()

        own = xb.at[p, c, y, x]
        own[:, pl.ds(0, EXT)] = ext[a]
        own[:, pl.ds(EXT, width)] = zin[a]
        own_a, own_b = own.at[:, col_a], own.at[:, col_b]
        rdma(own_a, own_a, ags.at[a, 0], agr.at[a, 0], to_xp).start()
        rdma(own_a, own_a, ags.at[a, 0], agr.at[a, 1], to_xm).start()
        rdma(own_b, own_b, ags.at[a, 0], agr.at[a, 2], to_yp).start()
        rdma(own_b, own_b, ags.at[a, 0], agr.at[a, 3], to_ym).start()
        rdma(own, own, ags.at[a, 4], agr.at[a, 16], to_peer).start()
        spread(a, p, x, y)

    def spread(a, p, bx, by):
        src_a, src_b = xb.at[p, c, y, bx, :, col_a], xb.at[p, c, by, x, :, col_b]
        rdma(src_a, src_a, ags.at[a, 2], agr.at[a, 8], to_yp).start()
        rdma(src_a, src_a, ags.at[a, 2], agr.at[a, 9], to_ym).start()
        rdma(src_b, src_b, ags.at[a, 2], agr.at[a, 10], to_xp).start()
        rdma(src_b, src_b, ags.at[a, 2], agr.at[a, 11], to_xm).start()

    def to_partner(a, ref):
        rdma(ref, ref, ags.at[a, 4], agr.at[a, 16], to_peer).start()

    def gather_2(a, p):
        left, right = xb.at[p, c, y, xm], xb.at[p, c, y, xp]
        below, above = xb.at[p, c, ym, x], xb.at[p, c, yp, x]
        wait_recv(left.at[:, col_a], agr.at[a, 0])
        rdma(left.at[:, col_q[0]], left.at[:, col_q[0]], ags.at[a, 1], agr.at[a, 4], to_xp).start()
        wait_recv(right.at[:, col_a], agr.at[a, 1])
        rdma(right.at[:, col_q[1]], right.at[:, col_q[1]], ags.at[a, 1], agr.at[a, 5], to_xm).start()
        wait_recv(below.at[:, col_b], agr.at[a, 2])
        rdma(below.at[:, col_q[2]], below.at[:, col_q[2]], ags.at[a, 1], agr.at[a, 6], to_yp).start()
        wait_recv(above.at[:, col_b], agr.at[a, 3])
        rdma(above.at[:, col_q[3]], above.at[:, col_q[3]], ags.at[a, 1], agr.at[a, 7], to_ym).start()
        spread(a, p, xm, ym)
        spread(a, p, xp, yp)
        for ref in (left.at[:, col_a], right.at[:, col_a], below.at[:, col_b], above.at[:, col_b]):
            to_partner(a, ref)

    def gather_3(a, p):
        across, over = xb.at[p, c, y, xd], xb.at[p, c, yd, x]
        wait_recv(across.at[:, col_q[0]], agr.at[a, 4])
        wait_recv(across.at[:, col_q[1]], agr.at[a, 5])
        wait_recv(over.at[:, col_q[2]], agr.at[a, 6])
        wait_recv(over.at[:, col_q[3]], agr.at[a, 7])
        spread(a, p, xd, yd)
        to_partner(a, across.at[:, col_a])
        to_partner(a, over.at[:, col_b])

    def gather_4(a, p):
        below, above = xb.at[p, c, ym], xb.at[p, c, yp]
        left, right = xb.at[p, c, :, xm], xb.at[p, c, :, xp]
        wait_recv(below.at[:, :, col_a], agr.at[a, 8])
        rdma(below.at[:, :, col_q[0]], below.at[:, :, col_q[0]], ags.at[a, 3], agr.at[a, 12], to_yp).start()
        wait_recv(above.at[:, :, col_a], agr.at[a, 9])
        rdma(above.at[:, :, col_q[1]], above.at[:, :, col_q[1]], ags.at[a, 3], agr.at[a, 13], to_ym).start()
        wait_recv(left.at[:, :, col_b], agr.at[a, 10])
        rdma(left.at[:, :, col_q[2]], left.at[:, :, col_q[2]], ags.at[a, 3], agr.at[a, 14], to_xp).start()
        wait_recv(right.at[:, :, col_b], agr.at[a, 11])
        rdma(right.at[:, :, col_q[3]], right.at[:, :, col_q[3]], ags.at[a, 3], agr.at[a, 15], to_xm).start()
        for ref in (below.at[:, :, col_a], above.at[:, :, col_a], left.at[:, :, col_b], right.at[:, :, col_b]):
            to_partner(a, ref)

    def gather_5(a, p):
        over, across = xb.at[p, c, yd], xb.at[p, c, :, xd]
        wait_recv(over.at[:, :, col_q[0]], agr.at[a, 12])
        wait_recv(over.at[:, :, col_q[1]], agr.at[a, 13])
        to_partner(a, over.at[:, :, col_a])
        wait_recv(across.at[:, :, col_q[2]], agr.at[a, 14])
        wait_recv(across.at[:, :, col_q[3]], agr.at[a, 15])
        to_partner(a, across.at[:, :, col_b])

    tokens = acc.shape[0]
    depth = quarter if quarter % 256 else quarter // 2

    def up(g, p):
        wait_recv(xb.at[p, co], agr.at[g, 16])

        def step(k, carry):
            at = pl.multiple_of(k * depth, 128)
            rows = xb[p, :, :, :, :, pl.ds(EXT + at, depth)].reshape(tokens, depth)
            term = jnp.dot(rows, wgu[pl.ds(at, depth), :], preferred_element_type=F32)
            acc[...] = jnp.where(k == 0, term, acc[...] + term)
            return carry

        lax.fori_loop(0, width // depth, step, 0)

        def activate(i, carry):
            fours = 4 * ROWS
            at = pl.multiple_of(i * fours, fours)
            coded = xb[p, lax.div(i, 4), lax.rem(i, 4), :, :, pl.ds(0, EXT)].reshape(fours, EXT).astype(F32)
            lanes = lax.broadcasted_iota(jnp.int32, coded.shape, 1)
            weight = jnp.sum(jnp.where(lax.rem(lanes, 8) == ey, coded, 0.0), axis=1, keepdims=True)
            first = acc[pl.ds(at, fours), pl.ds(0, units)]
            second = acc[pl.ds(at, fours), pl.ds(units, units)]
            value = first / (1.0 + jnp.exp(-first)) * second
            hid[pl.ds(at, fours), :] = (value * weight).astype(BF)
            return carry

        lax.fori_loop(0, tokens // (4 * ROWS), activate, 0)
        wait_send(xb.at[p, c, 0, pl.ds(0, 2)], ags.at[g, 0])
        wait_send(xb.at[p, c, 0, 0], ags.at[g, 1])
        wait_send(xb.at[p, c, pl.ds(0, 2)], ags.at[g, 2])
        wait_send(xb.at[p, c, 0], ags.at[g, 3])
        wait_send(xb.at[p, c], ags.at[g, 4])

        @pl.when(g < 2)
        def _():
            for device in (to_xp, to_xm, to_yp, to_ym, to_peer):
                pl.semaphore_signal(free_x.at[g], inc=1, device_id=device, device_id_type=MESH)

    def cols(q):
        return pl.ds(q * quarter, quarter)

    def pick(q, bx, by):
        return part.at[c, by, :, :, cols(q)] if q < 2 else part.at[c, :, bx, :, cols(q)]

    fwd = ((xp, yp), (xm, ym))
    bwd = ((xm, ym), (xp, yp))
    dev_first = ((to_yp, to_ym), (to_ym, to_yp), (to_xp, to_xm), (to_xm, to_xp))
    dev_second = ((to_xp, to_xm), (to_xm, to_xp), (to_yp, to_ym), (to_ym, to_yp))

    def down(g):
        @pl.when(g >= 1)
        def _():
            wait_send(part.at[co], pds.at[g - 1])
            pl.semaphore_wait(free_p.at[g - 1], 1)

        tile = 256
        side = tokens // 2
        rows_peer = pl.ds(pl.multiple_of(co * side, side), side)
        rows_mine = pl.ds(pl.multiple_of(c * side, side), side)
        for q in range(4):
            def step(j, carry):
                at = pl.multiple_of(q * quarter + j * tile, 128)
                value = jnp.dot(hid[rows_peer, :], wd[:, pl.ds(at, tile)], preferred_element_type=F32)
                part[co, :, :, :, pl.ds(at, tile)] = value.astype(BF).reshape(4, 4, ROWS, tile)
                return carry

            lax.fori_loop(0, quarter // tile, step, 0)
            rdma(part.at[co, :, :, :, cols(q)], peer.at[:, :, :, cols(q)], pds.at[g], prd.at[g, q], to_peer).start()

        @pl.when(g >= 1)
        def _():
            wait_send(part.at[c, pl.ds(0, 3)], rsend.at[g - 1])

        for q in range(4):
            wait_recv(peer.at[:, :, :, cols(q)], prd.at[g, q])

            def add(j, carry):
                at = pl.multiple_of(q * quarter + j * tile, 128)
                value = jnp.dot(hid[rows_mine, :], wd[:, pl.ds(at, tile)], preferred_element_type=F32)
                value = value + peer[:, :, :, pl.ds(at, tile)].reshape(side, tile).astype(F32)
                part[c, :, :, :, pl.ds(at, tile)] = value.astype(BF).reshape(4, 4, ROWS, tile)
                return carry

            lax.fori_loop(0, quarter // tile, add, 0)
            k = q % 2
            rdma(pick(q, xd, yd), rb.at[g, q, 0], rsend.at[g], relay.at[g, q], dev_first[q][0]).start()
            rdma(pick(q, *bwd[k]), rb.at[g, q, 1], rsend.at[g], meet.at[g, q], dev_first[q][1]).start()

        @pl.when(g < groups - 1)
        def _():
            pl.semaphore_signal(free_p.at[g], inc=1, device_id=to_peer, device_id_type=MESH)

    def scatter_2(g):
        for q in range(4):
            wait_recv(rb.at[g, q, 0], relay.at[g, q])
            mine = pick(q, *fwd[q % 2])

            def add(i, carry):
                mine[i] = (mine[i].astype(F32) + rb[g, q, 0, i].astype(F32)).astype(BF)
                return carry

            lax.fori_loop(0, 4, add, 0)
            rdma(mine, rb.at[g, q, 2], rsend.at[g], meet.at[g, q], dev_first[q][0]).start()

    def scatter_3(g):
        for q in range(4):
            wait_recv(rb.at[g, q, pl.ds(1, 2)], meet.at[g, q])
            mine = pick(q, x, y)

            def add(i, carry):
                total = mine[i].astype(F32) + rb[g, q, 1, i].astype(F32) + rb[g, q, 2, i].astype(F32)
                tot[q, i] = total.astype(BF)
                return carry

            lax.fori_loop(0, 4, add, 0)
            k = q % 2
            far, back = (xd, bwd[k][0]) if q < 2 else (yd, bwd[k][1])
            rdma(tot.at[q, far], rb2.at[g, q, 0], rsend2.at[g], relay2.at[g, q], dev_second[q][0]).start()
            rdma(tot.at[q, back], rb2.at[g, q, 1], rsend2.at[g], meet2.at[g, q], dev_second[q][1]).start()

    def scatter_4(g):
        for q in range(4):
            wait_recv(rb2.at[g, q, 0], relay2.at[g, q])
            at = fwd[q % 2][0] if q < 2 else fwd[q % 2][1]
            tot[q, at] = (tot[q, at].astype(F32) + rb2[g, q, 0].astype(F32)).astype(BF)
            rdma(tot.at[q, at], rb2.at[g, q, 2], rsend2.at[g], meet2.at[g, q], dev_second[q][0]).start()

    def scatter_5(g):
        rows = pl.ds(pl.multiple_of(g * ROWS, ROWS), ROWS)
        for q in range(4):
            wait_recv(rb2.at[g, q, pl.ds(1, 2)], meet2.at[g, q])
            at = x if q < 2 else y
            total = tot[q, at].astype(F32) + rb2[g, q, 1].astype(F32) + rb2[g, q, 2].astype(F32)
            out_ref[rows, cols(q)] = (total + zin[g, :, cols(q)].astype(F32)).astype(BF)
        wait_send(tot.at[pl.ds(0, 3)], rsend2.at[g])

    def turn(i, carry):
        a, n, g, t = i, i + 1, i - 1, i - 2
        pa, pn = lax.rem(i, 2), lax.rem(i + 1, 2)
        gathers, starts = a < groups, n < groups
        computes = (g >= 0) & (g < groups)
        ends = t >= 0

        @pl.when(computes)
        def _():
            up(g, pn)

        @pl.when(gathers)
        def _():
            gather_3(a, pa)

        @pl.when(ends)
        def _():
            scatter_3(t)

        @pl.when(computes)
        def _():
            down(g)

        @pl.when(gathers)
        def _():
            gather_4(a, pa)

        @pl.when(ends)
        def _():
            scatter_4(t)

        @pl.when(starts)
        def _():
            gather_1(n, pn)

        @pl.when(computes)
        def _():
            scatter_2(g)

        @pl.when(ends)
        def _():
            scatter_5(t)

        @pl.when(gathers)
        def _():
            gather_5(a, pa)

        @pl.when(starts)
        def _():
            gather_2(n, pn)

        return carry

    gather_1(0, 0)
    unpack(0, pieces // 2)
    gather_2(0, 0)
    unpack(pieces // 2, pieces - pieces // 2)
    load_d.wait()
    lax.fori_loop(0, groups + 2, turn, 0)
    wait_send(part.at[co], pds.at[groups - 1])
    wait_send(part.at[c, pl.ds(0, 3)], rsend.at[groups - 1])
    for g in range(groups):
        wait_send(zin.at[g], zsend.at[g])


def on_device(section_out, expert_ids, gate_weights, w_gate_up, w_down):
    rows, width = section_out.shape[1:]
    units = w_down.shape[2]
    groups = rows // ROWS
    quarter = width // 4
    hbm = pl.BlockSpec(memory_space=pl.ANY)
    vmem = pl.BlockSpec(memory_space=pltpu.VMEM)
    dma = pltpu.SemaphoreType.DMA
    regular = pltpu.SemaphoreType.REGULAR
    result = pl.pallas_call(
        moe_kernel,
        out_shape=jax.ShapeDtypeStruct((rows, width), BF),
        in_specs=[hbm, vmem, vmem, hbm, hbm],
        out_specs=vmem,
        scratch_shapes=[
            pltpu.VMEM((2, 2, 4, 4, ROWS, EXT + width), BF),
            pltpu.VMEM((groups, ROWS, width), BF),
            pltpu.VMEM((groups, ROWS, EXT), BF),
            pltpu.VMEM((2, width // 8, 2, units), BF),
            pltpu.VMEM((width, 2 * units), BF),
            pltpu.VMEM((units, width), BF),
            pltpu.VMEM((32 * ROWS, 2 * units), F32),
            pltpu.VMEM((32 * ROWS, units), BF),
            pltpu.VMEM((2, 4, 4, ROWS, width), BF),
            pltpu.VMEM((4, 4, ROWS, width), BF),
            pltpu.VMEM((groups, 4, 3, 4, ROWS, quarter), BF),
            pltpu.VMEM((4, 4, ROWS, quarter), BF),
            pltpu.VMEM((groups, 4, 3, ROWS, quarter), BF),
            dma((3,)), dma((groups,)), dma((groups,)),
            dma((groups, 17)), dma((groups, 5)),
            dma((groups, 4)), dma((groups,)),
            dma((groups, 4)), dma((groups, 4)), dma((groups,)),
            dma((groups, 4)), dma((groups, 4)), dma((groups,)),
            regular((groups,)), regular((groups,)),
        ],
        compiler_params=pltpu.CompilerParams(
            collective_id=0, has_side_effects=True, vmem_limit_bytes=66_000_000
        ),
        name="moe",
    )(section_out[0], expert_ids[0].T, gate_weights[0].T, w_gate_up[0, 0], w_down[0, 0])
    return result[None]


def solution(mesh):
    return jax.shard_map(
        on_device,
        mesh=mesh,
        in_specs=(
            P("section", ("ex", "ey"), None),
            P("section", ("ex", "ey"), None),
            P("section", ("ex", "ey"), None),
            P("section", "ey", None, None, "ex"),
            P("section", "ey", "ex", None),
        ),
        out_specs=P("section", ("ex", "ey"), None),
        check_vma=False,
    )
```

```python
import jax
import jax.numpy as jnp
from jax import lax
from jax.experimental import pallas as pl
from jax.experimental.pallas import tpu as pltpu
from jax.sharding import PartitionSpec as P

MESH = pl.DeviceIdType.MESH
ROWS = 16
EXT = 128
BF = jnp.bfloat16
F32 = jnp.float32


def moe_kernel(
    sec_ref, id_ref, gate_ref, wgu_hbm, wd_hbm, out_ref,
    xb, zin, ext, raw, wgu, wd, acc, hid, part, peer, rb, tot, rb2,
    wsem, zsend, zrecv, agr, ags, prd, pds, relay, meet, rsend, relay2, meet2, rsend2, free_x, free_p,
):
    groups = zin.shape[0]
    width = zin.shape[2]
    units = wd.shape[0]
    quarter = width // 4
    half = EXT + 2 * quarter
    whole = EXT + width
    col_a, col_b = pl.ds(0, half), pl.ds(half, 2 * quarter)
    col_q = (
        pl.ds(0, EXT + quarter), pl.ds(EXT + quarter, quarter),
        pl.ds(half, quarter), pl.ds(half + quarter, quarter),
    )
    sec = lax.axis_index("section")
    x = lax.axis_index("ex")
    ey = lax.axis_index("ey")
    y, c = lax.div(ey, 2), lax.rem(ey, 2)
    co = 1 - c
    n_sec = lax.axis_size("section")
    xp, xm, xd = lax.rem(x + 1, 4), lax.rem(x + 3, 4), lax.rem(x + 2, 4)
    yp, ym, yd = lax.rem(y + 1, 4), lax.rem(y + 3, 4), lax.rem(y + 2, 4)
    zp, zm = lax.rem(sec + 1, n_sec), lax.rem(sec + n_sec - 1, n_sec)
    to_xp, to_xm = (sec, xp, ey), (sec, xm, ey)
    to_yp, to_ym = (sec, x, yp * 2 + c), (sec, x, ym * 2 + c)
    to_peer = (sec, x, y * 2 + co)
    to_zp, to_zm = (zp, x, ey), (zm, x, ey)

    def rdma(src, dst, ssem, rsem, device):
        return pltpu.make_async_remote_copy(
            src_ref=src, dst_ref=dst, send_sem=ssem, recv_sem=rsem, device_id=device, device_id_type=MESH
        )

    def wait_recv(ref, sem):
        rdma(ref, ref, sem, sem, to_peer).wait_recv()

    def wait_send(ref, sem):
        rdma(ref, ref, sem, sem, to_peer).wait_send()

    barrier = pltpu.get_barrier_semaphore()
    for device in (to_xp, to_xm, to_yp, to_ym, to_peer, to_zp, to_zm):
        pl.semaphore_signal(barrier, inc=1, device_id=device, device_id_type=MESH)
    pl.semaphore_wait(barrier, 7)

    def relay_rows(g):
        rows = pl.ds(pl.multiple_of(g * ROWS, ROWS), ROWS)
        return rdma(sec_ref.at[rows], zin.at[g], zsend.at[g], zrecv.at[g], to_zp)

    relay_rows(0).start()
    pieces, piece = width // raw.shape[1], raw.shape[1]

    def load(k, slot):
        return pltpu.make_async_copy(wgu_hbm.at[pl.ds(k * piece, piece)], raw.at[slot], wsem.at[slot])

    load(0, 0).start()
    load(1, 1).start()
    load_d = pltpu.make_async_copy(wd_hbm, wd, wsem.at[2])
    load_d.start()

    row = lax.broadcasted_iota(jnp.int32, (EXT, EXT), 0)
    table = jnp.zeros((EXT, EXT), F32)
    ids = jnp.concatenate([id_ref[...]] * (EXT // id_ref.shape[1]), axis=1)
    weights = jnp.concatenate([gate_ref[...]] * (EXT // gate_ref.shape[1]), axis=1)
    for k in range(ids.shape[0]):
        table = table + jnp.where(lax.rem(row, 8) == ids[k : k + 1], weights[k : k + 1], 0.0)
    high = table.astype(BF).astype(F32)
    mid = (table - high).astype(BF).astype(F32)
    low = table - high - mid
    terms = jnp.where(row < 8, high, jnp.where(row < 16, mid, jnp.where(row < 24, low, 0.0)))
    ext[...] = terms.T[: groups * ROWS].astype(BF).reshape(ext.shape)

    def unpack(first, count):
        for k in range(first, first + count):
            slot = k % 2
            load(k, slot).wait()

            def step(j, carry):
                at = pl.multiple_of(j * 128, 128)
                to = pl.multiple_of(k * piece + j * 128, 128)
                wgu[pl.ds(to, 128), :] = raw[slot, pl.ds(at, 128)].reshape(128, wgu.shape[1])
                return carry

            lax.fori_loop(0, piece // 128, step, 0)
            if k + 2 < pieces:
                load(k + 2, slot).start()

    def gather_1(a, p):
        @pl.when(a >= 2)
        def _():
            pl.semaphore_wait(free_x.at[a - 2], 5)

        wait_recv(zin.at[a], zrecv.at[a])

        @pl.when(a + 1 < groups)
        def _():
            relay_rows(a + 1).start()

        own = xb.at[p, c, y, x]
        own[:, pl.ds(0, EXT)] = ext[a]
        own[:, pl.ds(EXT, width)] = zin[a]
        own_a, own_b = own.at[:, col_a], own.at[:, col_b]
        rdma(own_a, own_a, ags.at[a, 0], agr.at[a, 0], to_xp).start()
        rdma(own_a, own_a, ags.at[a, 0], agr.at[a, 1], to_xm).start()
        rdma(own_b, own_b, ags.at[a, 0], agr.at[a, 2], to_yp).start()
        rdma(own_b, own_b, ags.at[a, 0], agr.at[a, 3], to_ym).start()
        rdma(own, own, ags.at[a, 4], agr.at[a, 16], to_peer).start()
        spread(a, p, x, y)

    def spread(a, p, bx, by):
        src_a, src_b = xb.at[p, c, y, bx, :, col_a], xb.at[p, c, by, x, :, col_b]
        rdma(src_a, src_a, ags.at[a, 2], agr.at[a, 8], to_yp).start()
        rdma(src_a, src_a, ags.at[a, 2], agr.at[a, 9], to_ym).start()
        rdma(src_b, src_b, ags.at[a, 2], agr.at[a, 10], to_xp).start()
        rdma(src_b, src_b, ags.at[a, 2], agr.at[a, 11], to_xm).start()

    def to_partner(a, ref):
        rdma(ref, ref, ags.at[a, 4], agr.at[a, 16], to_peer).start()

    def gather_2(a, p):
        left, right = xb.at[p, c, y, xm], xb.at[p, c, y, xp]
        below, above = xb.at[p, c, ym, x], xb.at[p, c, yp, x]
        wait_recv(left.at[:, col_a], agr.at[a, 0])
        rdma(left.at[:, col_q[0]], left.at[:, col_q[0]], ags.at[a, 1], agr.at[a, 4], to_xp).start()
        wait_recv(right.at[:, col_a], agr.at[a, 1])
        rdma(right.at[:, col_q[1]], right.at[:, col_q[1]], ags.at[a, 1], agr.at[a, 5], to_xm).start()
        wait_recv(below.at[:, col_b], agr.at[a, 2])
        rdma(below.at[:, col_q[2]], below.at[:, col_q[2]], ags.at[a, 1], agr.at[a, 6], to_yp).start()
        wait_recv(above.at[:, col_b], agr.at[a, 3])
        rdma(above.at[:, col_q[3]], above.at[:, col_q[3]], ags.at[a, 1], agr.at[a, 7], to_ym).start()
        spread(a, p, xm, ym)
        spread(a, p, xp, yp)
        for ref in (left.at[:, col_a], right.at[:, col_a], below.at[:, col_b], above.at[:, col_b]):
            to_partner(a, ref)

    def gather_3(a, p):
        across, over = xb.at[p, c, y, xd], xb.at[p, c, yd, x]
        wait_recv(across.at[:, col_q[0]], agr.at[a, 4])
        wait_recv(across.at[:, col_q[1]], agr.at[a, 5])
        wait_recv(over.at[:, col_q[2]], agr.at[a, 6])
        wait_recv(over.at[:, col_q[3]], agr.at[a, 7])
        spread(a, p, xd, yd)
        to_partner(a, across.at[:, col_a])
        to_partner(a, over.at[:, col_b])

    def gather_4(a, p):
        below, above = xb.at[p, c, ym], xb.at[p, c, yp]
        left, right = xb.at[p, c, :, xm], xb.at[p, c, :, xp]
        wait_recv(below.at[:, :, col_a], agr.at[a, 8])
        rdma(below.at[:, :, col_q[0]], below.at[:, :, col_q[0]], ags.at[a, 3], agr.at[a, 12], to_yp).start()
        wait_recv(above.at[:, :, col_a], agr.at[a, 9])
        rdma(above.at[:, :, col_q[1]], above.at[:, :, col_q[1]], ags.at[a, 3], agr.at[a, 13], to_ym).start()
        wait_recv(left.at[:, :, col_b], agr.at[a, 10])
        rdma(left.at[:, :, col_q[2]], left.at[:, :, col_q[2]], ags.at[a, 3], agr.at[a, 14], to_xp).start()
        wait_recv(right.at[:, :, col_b], agr.at[a, 11])
        rdma(right.at[:, :, col_q[3]], right.at[:, :, col_q[3]], ags.at[a, 3], agr.at[a, 15], to_xm).start()
        for ref in (below.at[:, :, col_a], above.at[:, :, col_a], left.at[:, :, col_b], right.at[:, :, col_b]):
            to_partner(a, ref)

    def gather_5(a, p):
        over, across = xb.at[p, c, yd], xb.at[p, c, :, xd]
        wait_recv(over.at[:, :, col_q[0]], agr.at[a, 12])
        wait_recv(over.at[:, :, col_q[1]], agr.at[a, 13])
        to_partner(a, over.at[:, :, col_a])
        wait_recv(across.at[:, :, col_q[2]], agr.at[a, 14])
        wait_recv(across.at[:, :, col_q[3]], agr.at[a, 15])
        to_partner(a, across.at[:, :, col_b])

    tokens = acc.shape[0]
    depth = quarter

    def up(g, p):
        wait_recv(xb.at[p, co], agr.at[g, 16])

        def step(k, carry):
            at = pl.multiple_of(k * depth, 128)
            rows = xb[p, :, :, :, :, pl.ds(EXT + at, depth)].reshape(tokens, depth)
            term = jnp.dot(rows, wgu[pl.ds(at, depth), :], preferred_element_type=F32)
            acc[...] = jnp.where(k == 0, term, acc[...] + term)
            return carry

        lax.fori_loop(0, width // depth, step, 0)

        def activate(i, carry):
            fours = 4 * ROWS
            at = pl.multiple_of(i * fours, fours)
            coded = xb[p, lax.div(i, 4), lax.rem(i, 4), :, :, pl.ds(0, EXT)].reshape(fours, EXT).astype(F32)
            lanes = lax.broadcasted_iota(jnp.int32, coded.shape, 1)
            weight = jnp.sum(jnp.where(lax.rem(lanes, 8) == ey, coded, 0.0), axis=1, keepdims=True)
            first = acc[pl.ds(at, fours), pl.ds(0, units)]
            second = acc[pl.ds(at, fours), pl.ds(units, units)]
            value = first / (1.0 + jnp.exp(-first)) * second
            hid[pl.ds(at, fours), :] = (value * weight).astype(BF)
            return carry

        lax.fori_loop(0, tokens // (4 * ROWS), activate, 0)
        wait_send(xb.at[p, c, 0, pl.ds(0, 2)], ags.at[g, 0])
        wait_send(xb.at[p, c, 0, 0], ags.at[g, 1])
        wait_send(xb.at[p, c, pl.ds(0, 2)], ags.at[g, 2])
        wait_send(xb.at[p, c, 0], ags.at[g, 3])
        wait_send(xb.at[p, c], ags.at[g, 4])

        @pl.when(g < 2)
        def _():
            for device in (to_xp, to_xm, to_yp, to_ym, to_peer):
                pl.semaphore_signal(free_x.at[g], inc=1, device_id=device, device_id_type=MESH)

    def cols(q):
        return pl.ds(q * quarter, quarter)

    def pick(q, bx, by):
        return part.at[c, by, :, :, cols(q)] if q < 2 else part.at[c, :, bx, :, cols(q)]

    fwd = ((xp, yp), (xm, ym))
    bwd = ((xm, ym), (xp, yp))
    dev_first = ((to_yp, to_ym), (to_ym, to_yp), (to_xp, to_xm), (to_xm, to_xp))
    dev_second = ((to_xp, to_xm), (to_xm, to_xp), (to_yp, to_ym), (to_ym, to_yp))

    tile = 256
    side = tokens // 2

    def down_peer(g):
        @pl.when(g >= 1)
        def _():
            wait_send(part.at[co], pds.at[g - 1])
            pl.semaphore_wait(free_p.at[g - 1], 1)

        rows_peer = pl.ds(pl.multiple_of(co * side, side), side)
        for q in range(4):
            def step(j, carry):
                at = pl.multiple_of(q * quarter + j * tile, 128)
                value = jnp.dot(hid[rows_peer, :], wd[:, pl.ds(at, tile)], preferred_element_type=F32)
                part[co, :, :, :, pl.ds(at, tile)] = value.astype(BF).reshape(4, 4, ROWS, tile)
                return carry

            lax.fori_loop(0, quarter // tile, step, 0, unroll=True)
            rdma(part.at[co, :, :, :, cols(q)], peer.at[:, :, :, cols(q)], pds.at[g], prd.at[g, q], to_peer).start()

    def down_mine(g):
        @pl.when(g >= 1)
        def _():
            wait_send(part.at[c, pl.ds(0, 3)], rsend.at[g - 1])

        rows_mine = pl.ds(pl.multiple_of(c * side, side), side)

        for q in range(4):
            wait_recv(peer.at[:, :, :, cols(q)], prd.at[g, q])

            def add(j, carry):
                at = pl.multiple_of(q * quarter + j * tile, 128)
                value = jnp.dot(hid[rows_mine, :], wd[:, pl.ds(at, tile)], preferred_element_type=F32)
                value = value + peer[:, :, :, pl.ds(at, tile)].reshape(side, tile).astype(F32)
                part[c, :, :, :, pl.ds(at, tile)] = value.astype(BF).reshape(4, 4, ROWS, tile)
                return carry

            lax.fori_loop(0, quarter // tile, add, 0, unroll=True)
            rdma(pick(q, xd, yd), rb.at[g, q, 0], rsend.at[g], relay.at[g, q], dev_first[q][0]).start()
        for q in range(4):
            rdma(pick(q, *bwd[q % 2]), rb.at[g, q, 1], rsend.at[g], meet.at[g, q], dev_first[q][1]).start()

        @pl.when(g < groups - 1)
        def _():
            pl.semaphore_signal(free_p.at[g], inc=1, device_id=to_peer, device_id_type=MESH)

    def scatter_2(g):
        for q in range(4):
            wait_recv(rb.at[g, q, 0], relay.at[g, q])
            mine = pick(q, *fwd[q % 2])

            def add(i, carry):
                mine[i] = (mine[i].astype(F32) + rb[g, q, 0, i].astype(F32)).astype(BF)
                return carry

            lax.fori_loop(0, 4, add, 0)
            rdma(mine, rb.at[g, q, 2], rsend.at[g], meet.at[g, q], dev_first[q][0]).start()

    def scatter_3(g):
        for q in range(4):
            wait_recv(rb.at[g, q, pl.ds(1, 2)], meet.at[g, q])
            mine = pick(q, x, y)

            def add(i, carry):
                total = mine[i].astype(F32) + rb[g, q, 1, i].astype(F32) + rb[g, q, 2, i].astype(F32)
                tot[q, i] = total.astype(BF)
                return carry

            lax.fori_loop(0, 4, add, 0)
            far = xd if q < 2 else yd
            rdma(tot.at[q, far], rb2.at[g, q, 0], rsend2.at[g], relay2.at[g, q], dev_second[q][0]).start()
        for q in range(4):
            back = bwd[q % 2][0] if q < 2 else bwd[q % 2][1]
            rdma(tot.at[q, back], rb2.at[g, q, 1], rsend2.at[g], meet2.at[g, q], dev_second[q][1]).start()

    def scatter_4(g):
        for q in range(4):
            wait_recv(rb2.at[g, q, 0], relay2.at[g, q])
            at = fwd[q % 2][0] if q < 2 else fwd[q % 2][1]
            tot[q, at] = (tot[q, at].astype(F32) + rb2[g, q, 0].astype(F32)).astype(BF)
            rdma(tot.at[q, at], rb2.at[g, q, 2], rsend2.at[g], meet2.at[g, q], dev_second[q][0]).start()

    def scatter_5(g):
        rows = pl.ds(pl.multiple_of(g * ROWS, ROWS), ROWS)
        for q in range(4):
            wait_recv(rb2.at[g, q, pl.ds(1, 2)], meet2.at[g, q])
            at = x if q < 2 else y
            total = tot[q, at].astype(F32) + rb2[g, q, 1].astype(F32) + rb2[g, q, 2].astype(F32)
            out_ref[rows, cols(q)] = (total + zin[g, :, cols(q)].astype(F32)).astype(BF)
        wait_send(tot.at[pl.ds(0, 3)], rsend2.at[g])

    def turn(i, carry):
        def stage(act, g, *rest):
            @pl.when((g >= 0) & (g < groups))
            def _():
                act(g, *rest)

        here, other = lax.rem(i, 2), lax.rem(i + 1, 2)
        stage(gather_4, i - 1, other)
        stage(scatter_3, i - 3)
        stage(down_mine, i - 2)
        stage(gather_2, i, here)

        @pl.when(i == 0)
        def _():
            unpack(pieces // 2, pieces - pieces // 2)
            load_d.wait()

        stage(gather_5, i - 1, other)
        stage(gather_3, i, here)
        stage(scatter_4, i - 3)
        stage(up, i - 1, other)
        stage(scatter_2, i - 2)
        stage(scatter_5, i - 3)
        stage(gather_1, i + 1, other)
        stage(down_peer, i - 1)
        return carry

    gather_1(0, 0)
    unpack(0, pieces // 2)
    lax.fori_loop(0, groups + 3, turn, 0)
    wait_send(part.at[co], pds.at[groups - 1])
    wait_send(part.at[c, pl.ds(0, 3)], rsend.at[groups - 1])
    for g in range(groups):
        wait_send(zin.at[g], zsend.at[g])


def on_device(section_out, expert_ids, gate_weights, w_gate_up, w_down):
    rows, width = section_out.shape[1:]
    units = w_down.shape[2]
    groups = rows // ROWS
    quarter = width // 4
    hbm = pl.BlockSpec(memory_space=pl.ANY)
    vmem = pl.BlockSpec(memory_space=pltpu.VMEM)
    dma = pltpu.SemaphoreType.DMA
    regular = pltpu.SemaphoreType.REGULAR
    result = pl.pallas_call(
        moe_kernel,
        out_shape=jax.ShapeDtypeStruct((rows, width), BF),
        in_specs=[hbm, vmem, vmem, hbm, hbm],
        out_specs=vmem,
        scratch_shapes=[
            pltpu.VMEM((2, 2, 4, 4, ROWS, EXT + width), BF),
            pltpu.VMEM((groups, ROWS, width), BF),
            pltpu.VMEM((groups, ROWS, EXT), BF),
            pltpu.VMEM((2, width // 8, 2, units), BF),
            pltpu.VMEM((width, 2 * units), BF),
            pltpu.VMEM((units, width), BF),
            pltpu.VMEM((32 * ROWS, 2 * units), F32),
            pltpu.VMEM((32 * ROWS, units), BF),
            pltpu.VMEM((2, 4, 4, ROWS, width), BF),
            pltpu.VMEM((4, 4, ROWS, width), BF),
            pltpu.VMEM((groups, 4, 3, 4, ROWS, quarter), BF),
            pltpu.VMEM((4, 4, ROWS, quarter), BF),
            pltpu.VMEM((groups, 4, 3, ROWS, quarter), BF),
            dma((3,)), dma((groups,)), dma((groups,)),
            dma((groups, 17)), dma((groups, 5)),
            dma((groups, 4)), dma((groups,)),
            dma((groups, 4)), dma((groups, 4)), dma((groups,)),
            dma((groups, 4)), dma((groups, 4)), dma((groups,)),
            regular((groups,)), regular((groups,)),
        ],
        compiler_params=pltpu.CompilerParams(
            collective_id=0, has_side_effects=True, vmem_limit_bytes=62_000_000
        ),
        name="moe",
    )(section_out[0], expert_ids[0].T, gate_weights[0].T, w_gate_up[0, 0], w_down[0, 0])
    return result[None]


def solution(mesh):
    return jax.shard_map(
        on_device,
        mesh=mesh,
        in_specs=(
            P("section", ("ex", "ey"), None),
            P("section", ("ex", "ey"), None),
            P("section", ("ex", "ey"), None),
            P("section", "ey", None, None, "ex"),
            P("section", "ey", "ex", None),
        ),
        out_specs=P("section", ("ex", "ey"), None),
        check_vma=False,
    )
```

```python
import jax
import jax.numpy as jnp
from jax import lax
from jax.experimental import pallas as pl
from jax.experimental.pallas import tpu as pltpu
from jax.sharding import PartitionSpec as P

MESH = pl.DeviceIdType.MESH
ROWS = 16
EXT = 128
BF = jnp.bfloat16
F32 = jnp.float32


def moe_kernel(
    sec_ref, id_ref, gate_ref, wgu_hbm, wd_hbm, out_ref,
    xb, zin, zout, ext, raw, wgu, wd, acc, hid, part, peer, rb, tot, rb2,
    wsem, zsend, zrecv, agr, ags, prd, pds, relay, meet, comb, rsend, relay2, meet2, rsend2, free_x, free_p,
):
    groups = zin.shape[0]
    width = zin.shape[2]
    units = wd.shape[0]
    quarter = width // 4
    half = EXT + 2 * quarter
    whole = EXT + width
    col_a, col_b = pl.ds(0, half), pl.ds(half, 2 * quarter)
    col_q = (
        pl.ds(0, EXT + quarter), pl.ds(EXT + quarter, quarter),
        pl.ds(half, quarter), pl.ds(half + quarter, quarter),
    )
    sec = lax.axis_index("section")
    x = lax.axis_index("ex")
    ey = lax.axis_index("ey")
    y, c = lax.div(ey, 2), lax.rem(ey, 2)
    co = 1 - c
    n_sec = lax.axis_size("section")
    xp, xm, xd = lax.rem(x + 1, 4), lax.rem(x + 3, 4), lax.rem(x + 2, 4)
    yp, ym, yd = lax.rem(y + 1, 4), lax.rem(y + 3, 4), lax.rem(y + 2, 4)
    zp, zm = lax.rem(sec + 1, n_sec), lax.rem(sec + n_sec - 1, n_sec)
    to_xp, to_xm = (sec, xp, ey), (sec, xm, ey)
    to_yp, to_ym = (sec, x, yp * 2 + c), (sec, x, ym * 2 + c)
    to_peer = (sec, x, y * 2 + co)
    to_zp, to_zm = (zp, x, ey), (zm, x, ey)

    def rdma(src, dst, ssem, rsem, device):
        return pltpu.make_async_remote_copy(
            src_ref=src, dst_ref=dst, send_sem=ssem, recv_sem=rsem, device_id=device, device_id_type=MESH
        )

    def wait_recv(ref, sem):
        rdma(ref, ref, sem, sem, to_peer).wait_recv()

    def wait_send(ref, sem):
        rdma(ref, ref, sem, sem, to_peer).wait_send()

    stage_0 = pltpu.make_async_copy(sec_ref.at[pl.ds(0, ROWS)], zout, wsem.at[3])
    stage_0.start()
    barrier = pltpu.get_barrier_semaphore()
    for device in (to_xp, to_xm, to_yp, to_ym, to_peer, to_zp, to_zm):
        pl.semaphore_signal(barrier, inc=1, device_id=device, device_id_type=MESH)
    pl.semaphore_wait(barrier, 7)

    def relay_rows(g):
        rows = pl.ds(pl.multiple_of(g * ROWS, ROWS), ROWS)
        return rdma(sec_ref.at[rows], zin.at[g], zsend.at[g], zrecv.at[g], to_zp)

    stage_0.wait()
    rdma(zout, zin.at[0], zsend.at[0], zrecv.at[0], to_zp).start()
    pieces, piece = width // raw.shape[1], raw.shape[1]

    def load(k, slot):
        return pltpu.make_async_copy(wgu_hbm.at[pl.ds(k * piece, piece)], raw.at[slot], wsem.at[slot])

    load(0, 0).start()
    load(1, 1).start()
    load_d = pltpu.make_async_copy(wd_hbm, wd, wsem.at[2])
    load_d.start()

    row = lax.broadcasted_iota(jnp.int32, (EXT, EXT), 0)
    table = jnp.zeros((EXT, EXT), F32)
    ids = jnp.concatenate([id_ref[...]] * (EXT // id_ref.shape[1]), axis=1)
    weights = jnp.concatenate([gate_ref[...]] * (EXT // gate_ref.shape[1]), axis=1)
    for k in range(ids.shape[0]):
        table = table + jnp.where(lax.rem(row, 8) == ids[k : k + 1], weights[k : k + 1], 0.0)
    high = table.astype(BF).astype(F32)
    mid = (table - high).astype(BF).astype(F32)
    low = table - high - mid
    terms = jnp.where(row < 8, high, jnp.where(row < 16, mid, jnp.where(row < 24, low, 0.0)))
    ext[...] = terms.T[: groups * ROWS].astype(BF).reshape(ext.shape)

    def unpack(first, count):
        for k in range(first, first + count):
            slot = k % 2
            load(k, slot).wait()

            def step(j, carry):
                at = pl.multiple_of(j * 128, 128)
                to = pl.multiple_of(k * piece + j * 128, 128)
                wgu[pl.ds(to, 128), :] = raw[slot, pl.ds(at, 128)].reshape(128, wgu.shape[1])
                return carry

            lax.fori_loop(0, piece // 128, step, 0)
            if k + 2 < pieces:
                load(k + 2, slot).start()

    def gather_1(a, p):
        @pl.when(a >= 2)
        def _():
            pl.semaphore_wait(free_x.at[a - 2], 5)

        wait_recv(zin.at[a], zrecv.at[a])

        @pl.when(a + 1 < groups)
        def _():
            relay_rows(a + 1).start()

        own = xb.at[p, c, y, x]
        own[:, pl.ds(0, EXT)] = ext[a]
        own[:, pl.ds(EXT, width)] = zin[a]
        own_a, own_b = own.at[:, col_a], own.at[:, col_b]
        rdma(own_a, own_a, ags.at[a, 0], agr.at[a, 0], to_xp).start()
        rdma(own_a, own_a, ags.at[a, 0], agr.at[a, 1], to_xm).start()
        rdma(own_b, own_b, ags.at[a, 0], agr.at[a, 2], to_yp).start()
        rdma(own_b, own_b, ags.at[a, 0], agr.at[a, 3], to_ym).start()
        rdma(own, own, ags.at[a, 4], agr.at[a, 16], to_peer).start()
        spread(a, p, x, y)

    def spread(a, p, bx, by):
        src_a, src_b = xb.at[p, c, y, bx, :, col_a], xb.at[p, c, by, x, :, col_b]
        rdma(src_a, src_a, ags.at[a, 2], agr.at[a, 8], to_yp).start()
        rdma(src_a, src_a, ags.at[a, 2], agr.at[a, 9], to_ym).start()
        rdma(src_b, src_b, ags.at[a, 2], agr.at[a, 10], to_xp).start()
        rdma(src_b, src_b, ags.at[a, 2], agr.at[a, 11], to_xm).start()

    def to_partner(a, ref):
        rdma(ref, ref, ags.at[a, 4], agr.at[a, 16], to_peer).start()

    def gather_2(a, p):
        left, right = xb.at[p, c, y, xm], xb.at[p, c, y, xp]
        below, above = xb.at[p, c, ym, x], xb.at[p, c, yp, x]
        wait_recv(left.at[:, col_a], agr.at[a, 0])
        rdma(left.at[:, col_q[0]], left.at[:, col_q[0]], ags.at[a, 1], agr.at[a, 4], to_xp).start()
        wait_recv(right.at[:, col_a], agr.at[a, 1])
        rdma(right.at[:, col_q[1]], right.at[:, col_q[1]], ags.at[a, 1], agr.at[a, 5], to_xm).start()
        wait_recv(below.at[:, col_b], agr.at[a, 2])
        rdma(below.at[:, col_q[2]], below.at[:, col_q[2]], ags.at[a, 1], agr.at[a, 6], to_yp).start()
        wait_recv(above.at[:, col_b], agr.at[a, 3])
        rdma(above.at[:, col_q[3]], above.at[:, col_q[3]], ags.at[a, 1], agr.at[a, 7], to_ym).start()
        spread(a, p, xm, ym)
        spread(a, p, xp, yp)
        for ref in (left.at[:, col_a], right.at[:, col_a], below.at[:, col_b], above.at[:, col_b]):
            to_partner(a, ref)

    def gather_3(a, p):
        across, over = xb.at[p, c, y, xd], xb.at[p, c, yd, x]
        wait_recv(across.at[:, col_q[0]], agr.at[a, 4])
        wait_recv(across.at[:, col_q[1]], agr.at[a, 5])
        wait_recv(over.at[:, col_q[2]], agr.at[a, 6])
        wait_recv(over.at[:, col_q[3]], agr.at[a, 7])
        spread(a, p, xd, yd)
        to_partner(a, across.at[:, col_a])
        to_partner(a, over.at[:, col_b])

    def gather_4(a, p):
        below, above = xb.at[p, c, ym], xb.at[p, c, yp]
        left, right = xb.at[p, c, :, xm], xb.at[p, c, :, xp]
        wait_recv(below.at[:, :, col_a], agr.at[a, 8])
        rdma(below.at[:, :, col_q[0]], below.at[:, :, col_q[0]], ags.at[a, 3], agr.at[a, 12], to_yp).start()
        wait_recv(above.at[:, :, col_a], agr.at[a, 9])
        rdma(above.at[:, :, col_q[1]], above.at[:, :, col_q[1]], ags.at[a, 3], agr.at[a, 13], to_ym).start()
        wait_recv(left.at[:, :, col_b], agr.at[a, 10])
        rdma(left.at[:, :, col_q[2]], left.at[:, :, col_q[2]], ags.at[a, 3], agr.at[a, 14], to_xp).start()
        wait_recv(right.at[:, :, col_b], agr.at[a, 11])
        rdma(right.at[:, :, col_q[3]], right.at[:, :, col_q[3]], ags.at[a, 3], agr.at[a, 15], to_xm).start()
        for ref in (below.at[:, :, col_a], above.at[:, :, col_a], left.at[:, :, col_b], right.at[:, :, col_b]):
            to_partner(a, ref)

    def gather_5(a, p):
        over, across = xb.at[p, c, yd], xb.at[p, c, :, xd]
        wait_recv(over.at[:, :, col_q[0]], agr.at[a, 12])
        wait_recv(over.at[:, :, col_q[1]], agr.at[a, 13])
        to_partner(a, over.at[:, :, col_a])
        wait_recv(across.at[:, :, col_q[2]], agr.at[a, 14])
        wait_recv(across.at[:, :, col_q[3]], agr.at[a, 15])
        to_partner(a, across.at[:, :, col_b])

    tokens = acc.shape[0]
    depth = quarter

    def up(g, p):
        wait_recv(xb.at[p, co], agr.at[g, 16])

        def step(k, carry):
            at = pl.multiple_of(k * depth, 128)
            rows = xb[p, :, :, :, :, pl.ds(EXT + at, depth)].reshape(tokens, depth)
            term = jnp.dot(rows, wgu[pl.ds(at, depth), :], preferred_element_type=F32)
            acc[...] = jnp.where(k == 0, term, acc[...] + term)
            return carry

        lax.fori_loop(0, width // depth, step, 0)

        def activate(i, carry):
            fours = 4 * ROWS
            at = pl.multiple_of(i * fours, fours)
            coded = xb[p, lax.div(i, 4), lax.rem(i, 4), :, :, pl.ds(0, EXT)].reshape(fours, EXT).astype(F32)
            lanes = lax.broadcasted_iota(jnp.int32, coded.shape, 1)
            weight = jnp.sum(jnp.where(lax.rem(lanes, 8) == ey, coded, 0.0), axis=1, keepdims=True)
            first = acc[pl.ds(at, fours), pl.ds(0, units)]
            second = acc[pl.ds(at, fours), pl.ds(units, units)]
            value = first / (1.0 + jnp.exp(-first)) * second
            hid[pl.ds(at, fours), :] = (value * weight).astype(BF)
            return carry

        lax.fori_loop(0, tokens // (4 * ROWS), activate, 0)
        wait_send(xb.at[p, c, 0, pl.ds(0, 2)], ags.at[g, 0])
        wait_send(xb.at[p, c, 0, 0], ags.at[g, 1])
        wait_send(xb.at[p, c, pl.ds(0, 2)], ags.at[g, 2])
        wait_send(xb.at[p, c, 0], ags.at[g, 3])
        wait_send(xb.at[p, c], ags.at[g, 4])

        @pl.when(g < 2)
        def _():
            for device in (to_xp, to_xm, to_yp, to_ym, to_peer):
                pl.semaphore_signal(free_x.at[g], inc=1, device_id=device, device_id_type=MESH)

    def cols(q):
        return pl.ds(q * quarter, quarter)

    def pick(q, bx, by):
        return part.at[c, by, :, :, cols(q)] if q < 2 else part.at[c, :, bx, :, cols(q)]

    fwd = ((xp, yp), (xm, ym))
    bwd = ((xm, ym), (xp, yp))
    dev_first = ((to_yp, to_ym), (to_ym, to_yp), (to_xp, to_xm), (to_xm, to_xp))
    dev_second = ((to_xp, to_xm), (to_xm, to_xp), (to_yp, to_ym), (to_ym, to_yp))

    tile = 256
    side = tokens // 2

    def down_peer(g):
        @pl.when(g >= 1)
        def _():
            wait_send(part.at[co], pds.at[g - 1])
            pl.semaphore_wait(free_p.at[g - 1], 1)

        rows_peer = pl.ds(pl.multiple_of(co * side, side), side)
        for q in range(4):
            def step(j, carry):
                at = pl.multiple_of(q * quarter + j * tile, 128)
                value = jnp.dot(hid[rows_peer, :], wd[:, pl.ds(at, tile)], preferred_element_type=F32)
                part[co, :, :, :, pl.ds(at, tile)] = value.astype(BF).reshape(4, 4, ROWS, tile)
                return carry

            lax.fori_loop(0, quarter // tile, step, 0, unroll=True)
            rdma(part.at[co, :, :, :, cols(q)], peer.at[:, :, :, cols(q)], pds.at[g], prd.at[g, q], to_peer).start()

    def down_mine(g):
        @pl.when(g >= 1)
        def _():
            wait_send(part.at[c, pl.ds(0, 3)], rsend.at[g - 1])

        rows_mine = pl.ds(pl.multiple_of(c * side, side), side)

        for q in range(4):
            wait_recv(peer.at[:, :, :, cols(q)], prd.at[g, q])

            def add(j, carry):
                at = pl.multiple_of(q * quarter + j * tile, 128)
                value = jnp.dot(hid[rows_mine, :], wd[:, pl.ds(at, tile)], preferred_element_type=F32)
                value = value + peer[:, :, :, pl.ds(at, tile)].reshape(side, tile).astype(F32)
                part[c, :, :, :, pl.ds(at, tile)] = value.astype(BF).reshape(4, 4, ROWS, tile)
                return carry

            lax.fori_loop(0, quarter // tile, add, 0, unroll=True)
            rdma(pick(q, xd, yd), rb.at[g, q, 0], rsend.at[g], relay.at[g, q], dev_first[q][0]).start()
        for q in range(4):
            rdma(pick(q, *bwd[q % 2]), rb.at[g, q, 1], rsend.at[g], meet.at[g, q], dev_first[q][1]).start()

        @pl.when(g < groups - 1)
        def _():
            pl.semaphore_signal(free_p.at[g], inc=1, device_id=to_peer, device_id_type=MESH)

    def turns(q):
        k = q // 2
        return ((xd, yd)[k], bwd[q % 2][k], fwd[q % 2][k], (x, y)[k])

    def scatter_2(g):
        for q in range(4):
            wait_recv(rb.at[g, q, 0], relay.at[g, q])
            mine = pick(q, *fwd[q % 2])

            def add(i, carry):
                mine[i] = (mine[i].astype(F32) + rb[g, q, 0, i].astype(F32)).astype(BF)
                return carry

            lax.fori_loop(0, 4, add, 0)
            for k, at in enumerate(turns(q)):
                rdma(mine.at[at], rb.at[g, q, 2, at], rsend.at[g], comb.at[g, q, k], dev_first[q][0]).start()

    def scatter_3(g):
        def settle(q, k):
            at = turns(q)[k]
            wait_recv(rb.at[g, q, 2, at], comb.at[g, q, k])
            mine = pick(q, x, y)
            total = mine[at].astype(F32) + rb[g, q, 1, at].astype(F32) + rb[g, q, 2, at].astype(F32)
            tot[q, at] = total.astype(BF)
            return tot.at[q, at]

        for q in range(4):
            wait_recv(rb.at[g, q, 1], meet.at[g, q])
            rdma(settle(q, 0), rb2.at[g, q, 0], rsend2.at[g], relay2.at[g, q], dev_second[q][0]).start()
        for q in range(4):
            rdma(settle(q, 1), rb2.at[g, q, 1], rsend2.at[g], meet2.at[g, q], dev_second[q][1]).start()
        for q in range(4):
            settle(q, 2)
            settle(q, 3)

    def scatter_4(g):
        for q in range(4):
            wait_recv(rb2.at[g, q, 0], relay2.at[g, q])
            at = fwd[q % 2][0] if q < 2 else fwd[q % 2][1]
            tot[q, at] = (tot[q, at].astype(F32) + rb2[g, q, 0].astype(F32)).astype(BF)
            rdma(tot.at[q, at], rb2.at[g, q, 2], rsend2.at[g], meet2.at[g, q], dev_second[q][0]).start()

    def scatter_5(g):
        rows = pl.ds(pl.multiple_of(g * ROWS, ROWS), ROWS)
        for q in range(4):
            wait_recv(rb2.at[g, q, pl.ds(1, 2)], meet2.at[g, q])
            at = x if q < 2 else y
            total = tot[q, at].astype(F32) + rb2[g, q, 1].astype(F32) + rb2[g, q, 2].astype(F32)
            out_ref[rows, cols(q)] = (total + zin[g, :, cols(q)].astype(F32)).astype(BF)
        wait_send(tot.at[pl.ds(0, 3)], rsend2.at[g])

    def turn(i, carry):
        def stage(act, g, *rest):
            @pl.when((g >= 0) & (g < groups))
            def _():
                act(g, *rest)

        here, other = lax.rem(i, 2), lax.rem(i + 1, 2)
        stage(gather_4, i - 1, other)
        stage(scatter_3, i - 3)
        stage(gather_2, i, here)

        @pl.when(i == 0)
        def _():
            unpack(pieces // 2, pieces - pieces // 2)
            load_d.wait()

        stage(down_mine, i - 2)
        stage(gather_5, i - 1, other)
        stage(gather_3, i, here)
        stage(scatter_4, i - 3)
        stage(up, i - 1, other)
        stage(scatter_2, i - 2)
        stage(gather_1, i + 1, other)
        stage(down_peer, i - 1)
        stage(scatter_5, i - 3)
        return carry

    gather_1(0, 0)
    unpack(0, pieces // 2)
    lax.fori_loop(0, groups + 3, turn, 0)
    wait_send(part.at[co], pds.at[groups - 1])
    wait_send(part.at[c, pl.ds(0, 3)], rsend.at[groups - 1])
    for g in range(groups):
        wait_send(zin.at[g], zsend.at[g])


def on_device(section_out, expert_ids, gate_weights, w_gate_up, w_down):
    rows, width = section_out.shape[1:]
    units = w_down.shape[2]
    groups = rows // ROWS
    quarter = width // 4
    hbm = pl.BlockSpec(memory_space=pl.ANY)
    vmem = pl.BlockSpec(memory_space=pltpu.VMEM)
    dma = pltpu.SemaphoreType.DMA
    regular = pltpu.SemaphoreType.REGULAR
    result = pl.pallas_call(
        moe_kernel,
        out_shape=jax.ShapeDtypeStruct((rows, width), BF),
        in_specs=[hbm, vmem, vmem, hbm, hbm],
        out_specs=vmem,
        scratch_shapes=[
            pltpu.VMEM((2, 2, 4, 4, ROWS, EXT + width), BF),
            pltpu.VMEM((groups, ROWS, width), BF),
            pltpu.VMEM((ROWS, width), BF),
            pltpu.VMEM((groups, ROWS, EXT), BF),
            pltpu.VMEM((2, width // 8, 2, units), BF),
            pltpu.VMEM((width, 2 * units), BF),
            pltpu.VMEM((units, width), BF),
            pltpu.VMEM((32 * ROWS, 2 * units), F32),
            pltpu.VMEM((32 * ROWS, units), BF),
            pltpu.VMEM((2, 4, 4, ROWS, width), BF),
            pltpu.VMEM((4, 4, ROWS, width), BF),
            pltpu.VMEM((groups, 4, 3, 4, ROWS, quarter), BF),
            pltpu.VMEM((4, 4, ROWS, quarter), BF),
            pltpu.VMEM((groups, 4, 3, ROWS, quarter), BF),
            dma((4,)), dma((groups,)), dma((groups,)),
            dma((groups, 17)), dma((groups, 5)),
            dma((groups, 4)), dma((groups,)),
            dma((groups, 4)), dma((groups, 4)), dma((groups, 4, 4)), dma((groups,)),
            dma((groups, 4)), dma((groups, 4)), dma((groups,)),
            regular((groups,)), regular((groups,)),
        ],
        compiler_params=pltpu.CompilerParams(
            collective_id=0, has_side_effects=True, vmem_limit_bytes=58_500_000
        ),
        name="moe",
    )(section_out[0], expert_ids[0].T, gate_weights[0].T, w_gate_up[0, 0], w_down[0, 0])
    return result[None]


def solution(mesh):
    return jax.shard_map(
        on_device,
        mesh=mesh,
        in_specs=(
            P("section", ("ex", "ey"), None),
            P("section", ("ex", "ey"), None),
            P("section", ("ex", "ey"), None),
            P("section", "ey", None, None, "ex"),
            P("section", "ey", "ex", None),
        ),
        out_specs=P("section", ("ex", "ey"), None),
        check_vma=False,
    )
```

```python
import jax
import jax.numpy as jnp
from jax import lax
from jax.experimental import pallas as pl
from jax.experimental.pallas import tpu as pltpu
from jax.sharding import PartitionSpec as P

MESH = pl.DeviceIdType.MESH
ROWS = 16
EXT = 128
BF = jnp.bfloat16
F32 = jnp.float32


def moe_kernel(
    sec_ref, id_ref, gate_ref, wgu_hbm, wd_hbm, out_ref,
    xb, zin, zout, ext, raw, wgu, wd, acc, hid, part, peer, rb, tot, rb2,
    wsem, zsend, zrecv, agr, ags, prd, pds, relay, meet, comb, rsend, relay2, meet2, rsend2, free_x, free_p,
):
    groups = zin.shape[0]
    width = zin.shape[2]
    units = wd.shape[0]
    quarter = width // 4
    half = EXT + 2 * quarter
    whole = EXT + width
    col_a, col_b = pl.ds(0, half), pl.ds(half, 2 * quarter)
    col_q = (
        pl.ds(0, EXT + quarter), pl.ds(EXT + quarter, quarter),
        pl.ds(half, quarter), pl.ds(half + quarter, quarter),
    )
    sec = lax.axis_index("section")
    x = lax.axis_index("ex")
    ey = lax.axis_index("ey")
    y, c = lax.div(ey, 2), lax.rem(ey, 2)
    co = 1 - c
    n_sec = lax.axis_size("section")
    xp, xm, xd = lax.rem(x + 1, 4), lax.rem(x + 3, 4), lax.rem(x + 2, 4)
    yp, ym, yd = lax.rem(y + 1, 4), lax.rem(y + 3, 4), lax.rem(y + 2, 4)
    zp, zm = lax.rem(sec + 1, n_sec), lax.rem(sec + n_sec - 1, n_sec)
    to_xp, to_xm = (sec, xp, ey), (sec, xm, ey)
    to_yp, to_ym = (sec, x, yp * 2 + c), (sec, x, ym * 2 + c)
    to_peer = (sec, x, y * 2 + co)
    to_zp, to_zm = (zp, x, ey), (zm, x, ey)

    def rdma(src, dst, ssem, rsem, device):
        return pltpu.make_async_remote_copy(
            src_ref=src, dst_ref=dst, send_sem=ssem, recv_sem=rsem, device_id=device, device_id_type=MESH
        )

    def wait_recv(ref, sem):
        rdma(ref, ref, sem, sem, to_peer).wait_recv()

    def wait_send(ref, sem):
        rdma(ref, ref, sem, sem, to_peer).wait_send()

    stage_0 = pltpu.make_async_copy(sec_ref.at[pl.ds(0, ROWS)], zout, wsem.at[3])
    stage_0.start()
    barrier = pltpu.get_barrier_semaphore()
    for device in (to_xp, to_xm, to_yp, to_ym, to_peer, to_zp, to_zm):
        pl.semaphore_signal(barrier, inc=1, device_id=device, device_id_type=MESH)
    pl.semaphore_wait(barrier, 7)

    def relay_rows(g):
        rows = pl.ds(pl.multiple_of(g * ROWS, ROWS), ROWS)
        return rdma(sec_ref.at[rows], zin.at[g], zsend.at[g], zrecv.at[g], to_zp)

    stage_0.wait()
    first, last = pl.ds(0, 2 * quarter), pl.ds(2 * quarter, 2 * quarter)
    rdma(zout.at[:, first], zin.at[0, :, first], zsend.at[0], zrecv.at[0], to_zp).start()
    rdma(zout.at[:, last], zin.at[0, :, last], zsend.at[0], zrecv.at[groups], to_zp).start()
    pieces, piece = width // raw.shape[1], raw.shape[1]

    def load(k, slot):
        return pltpu.make_async_copy(wgu_hbm.at[pl.ds(k * piece, piece)], raw.at[slot], wsem.at[slot])

    load(0, 0).start()
    load(1, 1).start()
    load_d = pltpu.make_async_copy(wd_hbm, wd, wsem.at[2])
    load_d.start()

    row = lax.broadcasted_iota(jnp.int32, (EXT, EXT), 0)
    table = jnp.zeros((EXT, EXT), F32)
    ids = jnp.concatenate([id_ref[...]] * (EXT // id_ref.shape[1]), axis=1)
    weights = jnp.concatenate([gate_ref[...]] * (EXT // gate_ref.shape[1]), axis=1)
    for k in range(ids.shape[0]):
        table = table + jnp.where(lax.rem(row, 8) == ids[k : k + 1], weights[k : k + 1], 0.0)
    high = table.astype(BF).astype(F32)
    mid = (table - high).astype(BF).astype(F32)
    low = table - high - mid
    terms = jnp.where(row < 8, high, jnp.where(row < 16, mid, jnp.where(row < 24, low, 0.0)))
    ext[...] = terms.T[: groups * ROWS].astype(BF).reshape(ext.shape)

    def unpack(first, count):
        for k in range(first, first + count):
            slot = k % 2
            load(k, slot).wait()

            def step(j, carry):
                at = pl.multiple_of(j * 128, 128)
                to = pl.multiple_of(k * piece + j * 128, 128)
                wgu[pl.ds(to, 128), :] = raw[slot, pl.ds(at, 128)].reshape(128, wgu.shape[1])
                return carry

            lax.fori_loop(0, piece // 128, step, 0)
            if k + 2 < pieces:
                load(k + 2, slot).start()

    def gather_1(a, p):
        @pl.when(a >= 2)
        def _():
            pl.semaphore_wait(free_x.at[a - 2], 5)

        wait_recv(zin.at[a], zrecv.at[a])

        @pl.when(a + 1 < groups)
        def _():
            relay_rows(a + 1).start()

        own = xb.at[p, c, y, x]
        own[:, pl.ds(0, EXT)] = ext[a]
        own[:, pl.ds(EXT, width)] = zin[a]
        own_a, own_b = own.at[:, col_a], own.at[:, col_b]
        rdma(own_a, own_a, ags.at[a, 0], agr.at[a, 0], to_xp).start()
        rdma(own_a, own_a, ags.at[a, 0], agr.at[a, 1], to_xm).start()
        rdma(own_b, own_b, ags.at[a, 0], agr.at[a, 2], to_yp).start()
        rdma(own_b, own_b, ags.at[a, 0], agr.at[a, 3], to_ym).start()
        rdma(own, own, ags.at[a, 4], agr.at[a, 16], to_peer).start()
        spread(a, p, x, y)

    def gather_1_first():
        own = xb.at[0, c, y, x]
        own_a, own_b = own.at[:, col_a], own.at[:, col_b]
        wait_recv(zin.at[0, :, first], zrecv.at[0])
        own[:, pl.ds(0, EXT)] = ext[0]
        own[:, pl.ds(EXT, 2 * quarter)] = zin[0, :, first]
        rdma(own_a, own_a, ags.at[0, 0], agr.at[0, 0], to_xp).start()
        rdma(own_a, own_a, ags.at[0, 0], agr.at[0, 1], to_xm).start()
        rdma(own_a, own_a, ags.at[0, 2], agr.at[0, 8], to_yp).start()
        rdma(own_a, own_a, ags.at[0, 2], agr.at[0, 9], to_ym).start()
        wait_recv(zin.at[0, :, last], zrecv.at[groups])
        relay_rows(1).start()
        own[:, col_b] = zin[0, :, last]
        rdma(own_b, own_b, ags.at[0, 0], agr.at[0, 2], to_yp).start()
        rdma(own_b, own_b, ags.at[0, 0], agr.at[0, 3], to_ym).start()
        rdma(own_b, own_b, ags.at[0, 2], agr.at[0, 10], to_xp).start()
        rdma(own_b, own_b, ags.at[0, 2], agr.at[0, 11], to_xm).start()
        rdma(own, own, ags.at[0, 4], agr.at[0, 16], to_peer).start()

    def spread(a, p, bx, by):
        src_a, src_b = xb.at[p, c, y, bx, :, col_a], xb.at[p, c, by, x, :, col_b]
        rdma(src_a, src_a, ags.at[a, 2], agr.at[a, 8], to_yp).start()
        rdma(src_a, src_a, ags.at[a, 2], agr.at[a, 9], to_ym).start()
        rdma(src_b, src_b, ags.at[a, 2], agr.at[a, 10], to_xp).start()
        rdma(src_b, src_b, ags.at[a, 2], agr.at[a, 11], to_xm).start()

    def to_partner(a, ref):
        rdma(ref, ref, ags.at[a, 4], agr.at[a, 16], to_peer).start()

    def gather_2(a, p):
        left, right = xb.at[p, c, y, xm], xb.at[p, c, y, xp]
        below, above = xb.at[p, c, ym, x], xb.at[p, c, yp, x]
        wait_recv(left.at[:, col_a], agr.at[a, 0])
        rdma(left.at[:, col_q[0]], left.at[:, col_q[0]], ags.at[a, 1], agr.at[a, 4], to_xp).start()
        wait_recv(right.at[:, col_a], agr.at[a, 1])
        rdma(right.at[:, col_q[1]], right.at[:, col_q[1]], ags.at[a, 1], agr.at[a, 5], to_xm).start()
        wait_recv(below.at[:, col_b], agr.at[a, 2])
        rdma(below.at[:, col_q[2]], below.at[:, col_q[2]], ags.at[a, 1], agr.at[a, 6], to_yp).start()
        wait_recv(above.at[:, col_b], agr.at[a, 3])
        rdma(above.at[:, col_q[3]], above.at[:, col_q[3]], ags.at[a, 1], agr.at[a, 7], to_ym).start()
        spread(a, p, xm, ym)
        spread(a, p, xp, yp)
        for ref in (left.at[:, col_a], right.at[:, col_a], below.at[:, col_b], above.at[:, col_b]):
            to_partner(a, ref)

    def gather_3(a, p):
        across, over = xb.at[p, c, y, xd], xb.at[p, c, yd, x]
        wait_recv(across.at[:, col_q[0]], agr.at[a, 4])
        wait_recv(across.at[:, col_q[1]], agr.at[a, 5])
        wait_recv(over.at[:, col_q[2]], agr.at[a, 6])
        wait_recv(over.at[:, col_q[3]], agr.at[a, 7])
        spread(a, p, xd, yd)
        to_partner(a, across.at[:, col_a])
        to_partner(a, over.at[:, col_b])

    def gather_4(a, p):
        below, above = xb.at[p, c, ym], xb.at[p, c, yp]
        left, right = xb.at[p, c, :, xm], xb.at[p, c, :, xp]
        wait_recv(below.at[:, :, col_a], agr.at[a, 8])
        rdma(below.at[:, :, col_q[0]], below.at[:, :, col_q[0]], ags.at[a, 3], agr.at[a, 12], to_yp).start()
        wait_recv(above.at[:, :, col_a], agr.at[a, 9])
        rdma(above.at[:, :, col_q[1]], above.at[:, :, col_q[1]], ags.at[a, 3], agr.at[a, 13], to_ym).start()
        wait_recv(left.at[:, :, col_b], agr.at[a, 10])
        rdma(left.at[:, :, col_q[2]], left.at[:, :, col_q[2]], ags.at[a, 3], agr.at[a, 14], to_xp).start()
        wait_recv(right.at[:, :, col_b], agr.at[a, 11])
        rdma(right.at[:, :, col_q[3]], right.at[:, :, col_q[3]], ags.at[a, 3], agr.at[a, 15], to_xm).start()
        for ref in (below.at[:, :, col_a], above.at[:, :, col_a], left.at[:, :, col_b], right.at[:, :, col_b]):
            to_partner(a, ref)

    def gather_5(a, p):
        over, across = xb.at[p, c, yd], xb.at[p, c, :, xd]
        wait_recv(over.at[:, :, col_q[0]], agr.at[a, 12])
        wait_recv(over.at[:, :, col_q[1]], agr.at[a, 13])
        to_partner(a, over.at[:, :, col_a])
        wait_recv(across.at[:, :, col_q[2]], agr.at[a, 14])
        wait_recv(across.at[:, :, col_q[3]], agr.at[a, 15])
        to_partner(a, across.at[:, :, col_b])

    tokens = acc.shape[0]
    depth = quarter

    def up(g, p):
        wait_recv(xb.at[p, co], agr.at[g, 16])

        def step(k, carry):
            at = pl.multiple_of(k * depth, 128)
            rows = xb[p, :, :, :, :, pl.ds(EXT + at, depth)].reshape(tokens, depth)
            term = jnp.dot(rows, wgu[pl.ds(at, depth), :], preferred_element_type=F32)
            acc[...] = jnp.where(k == 0, term, acc[...] + term)
            return carry

        lax.fori_loop(0, width // depth, step, 0, unroll=2)

        def activate(i, carry):
            fours = 4 * ROWS
            at = pl.multiple_of(i * fours, fours)
            coded = xb[p, lax.div(i, 4), lax.rem(i, 4), :, :, pl.ds(0, EXT)].reshape(fours, EXT).astype(F32)
            lanes = lax.broadcasted_iota(jnp.int32, coded.shape, 1)
            weight = jnp.sum(jnp.where(lax.rem(lanes, 8) == ey, coded, 0.0), axis=1, keepdims=True)
            first = acc[pl.ds(at, fours), pl.ds(0, units)]
            second = acc[pl.ds(at, fours), pl.ds(units, units)]
            value = first / (1.0 + jnp.exp(-first)) * second
            hid[pl.ds(at, fours), :] = (value * weight).astype(BF)
            return carry

        lax.fori_loop(0, tokens // (4 * ROWS), activate, 0, unroll=2)
        wait_send(xb.at[p, c, 0, pl.ds(0, 2)], ags.at[g, 0])
        wait_send(xb.at[p, c, 0, 0], ags.at[g, 1])
        wait_send(xb.at[p, c, pl.ds(0, 2)], ags.at[g, 2])
        wait_send(xb.at[p, c, 0], ags.at[g, 3])
        wait_send(xb.at[p, c], ags.at[g, 4])

        @pl.when(g < 2)
        def _():
            for device in (to_xp, to_xm, to_yp, to_ym, to_peer):
                pl.semaphore_signal(free_x.at[g], inc=1, device_id=device, device_id_type=MESH)

    def cols(q):
        return pl.ds(q * quarter, quarter)

    def pick(q, bx, by):
        return part.at[c, by, :, :, cols(q)] if q < 2 else part.at[c, :, bx, :, cols(q)]

    fwd = ((xp, yp), (xm, ym))
    bwd = ((xm, ym), (xp, yp))
    dev_first = ((to_yp, to_ym), (to_ym, to_yp), (to_xp, to_xm), (to_xm, to_xp))
    dev_second = ((to_xp, to_xm), (to_xm, to_xp), (to_yp, to_ym), (to_ym, to_yp))

    tile = 256
    side = tokens // 2

    def down_peer(g):
        @pl.when(g >= 1)
        def _():
            wait_send(part.at[co], pds.at[g - 1])
            pl.semaphore_wait(free_p.at[g - 1], 1)

        rows_peer = pl.ds(pl.multiple_of(co * side, side), side)
        for q in range(4):
            def step(j, carry):
                at = pl.multiple_of(q * quarter + j * tile, 128)
                value = jnp.dot(hid[rows_peer, :], wd[:, pl.ds(at, tile)], preferred_element_type=F32)
                part[co, :, :, :, pl.ds(at, tile)] = value.astype(BF).reshape(4, 4, ROWS, tile)
                return carry

            lax.fori_loop(0, quarter // tile, step, 0, unroll=True)
            rdma(part.at[co, :, :, :, cols(q)], peer.at[:, :, :, cols(q)], pds.at[g], prd.at[g, q], to_peer).start()

    def down_mine(g):
        @pl.when(g >= 1)
        def _():
            wait_send(part.at[c, pl.ds(0, 3)], rsend.at[g - 1])

        rows_mine = pl.ds(pl.multiple_of(c * side, side), side)

        for q in range(4):
            wait_recv(peer.at[:, :, :, cols(q)], prd.at[g, q])

            def add(j, carry):
                at = pl.multiple_of(q * quarter + j * tile, 128)
                value = jnp.dot(hid[rows_mine, :], wd[:, pl.ds(at, tile)], preferred_element_type=F32)
                value = value + peer[:, :, :, pl.ds(at, tile)].reshape(side, tile).astype(F32)
                part[c, :, :, :, pl.ds(at, tile)] = value.astype(BF).reshape(4, 4, ROWS, tile)
                return carry

            lax.fori_loop(0, quarter // tile, add, 0, unroll=True)
            rdma(pick(q, xd, yd), rb.at[g, q, 0], rsend.at[g], relay.at[g, q], dev_first[q][0]).start()
        for q in range(4):
            rdma(pick(q, *bwd[q % 2]), rb.at[g, q, 1], rsend.at[g], meet.at[g, q], dev_first[q][1]).start()

        @pl.when(g < groups - 1)
        def _():
            pl.semaphore_signal(free_p.at[g], inc=1, device_id=to_peer, device_id_type=MESH)

    def turns(q):
        k = q // 2
        return ((xd, yd)[k], bwd[q % 2][k], fwd[q % 2][k], (x, y)[k])

    def scatter_2(g):
        for q in range(4):
            wait_recv(rb.at[g, q, 0], relay.at[g, q])
            mine = pick(q, *fwd[q % 2])

            def add(i, carry):
                mine[i] = (mine[i].astype(F32) + rb[g, q, 0, i].astype(F32)).astype(BF)
                return carry

            lax.fori_loop(0, 4, add, 0)
            for k, at in enumerate(turns(q)):
                rdma(mine.at[at], rb.at[g, q, 2, at], rsend.at[g], comb.at[g, q, k], dev_first[q][0]).start()

    def scatter_3(g):
        def settle(q, k):
            at = turns(q)[k]
            wait_recv(rb.at[g, q, 2, at], comb.at[g, q, k])
            mine = pick(q, x, y)
            total = mine[at].astype(F32) + rb[g, q, 1, at].astype(F32) + rb[g, q, 2, at].astype(F32)
            tot[q, at] = total.astype(BF)
            return tot.at[q, at]

        for q in range(4):
            wait_recv(rb.at[g, q, 1], meet.at[g, q])
            rdma(settle(q, 0), rb2.at[g, q, 0], rsend2.at[g], relay2.at[g, q], dev_second[q][0]).start()
        for q in range(4):
            rdma(settle(q, 1), rb2.at[g, q, 1], rsend2.at[g], meet2.at[g, q], dev_second[q][1]).start()
        for q in range(4):
            settle(q, 2)
            settle(q, 3)

    def scatter_4(g):
        for q in range(4):
            wait_recv(rb2.at[g, q, 0], relay2.at[g, q])
            at = fwd[q % 2][0] if q < 2 else fwd[q % 2][1]
            tot[q, at] = (tot[q, at].astype(F32) + rb2[g, q, 0].astype(F32)).astype(BF)
            rdma(tot.at[q, at], rb2.at[g, q, 2], rsend2.at[g], meet2.at[g, q], dev_second[q][0]).start()

    def scatter_5(g):
        rows = pl.ds(pl.multiple_of(g * ROWS, ROWS), ROWS)
        for q in range(4):
            wait_recv(rb2.at[g, q, pl.ds(1, 2)], meet2.at[g, q])
            at = x if q < 2 else y
            total = tot[q, at].astype(F32) + rb2[g, q, 1].astype(F32) + rb2[g, q, 2].astype(F32)
            out_ref[rows, cols(q)] = (total + zin[g, :, cols(q)].astype(F32)).astype(BF)
        wait_send(tot.at[pl.ds(0, 3)], rsend2.at[g])

    def turn(i, carry):
        def stage(act, g, *rest):
            @pl.when((g >= 0) & (g < groups))
            def _():
                act(g, *rest)

        here, other = lax.rem(i, 2), lax.rem(i + 1, 2)
        stage(gather_4, i - 1, other)
        stage(scatter_3, i - 3)
        stage(gather_2, i, here)

        @pl.when(i == 0)
        def _():
            unpack(pieces // 2, pieces - pieces // 2)
            load_d.wait()

        stage(down_mine, i - 2)
        stage(gather_5, i - 1, other)
        stage(gather_3, i, here)
        stage(scatter_4, i - 3)
        stage(scatter_2, i - 2)
        stage(up, i - 1, other)
        stage(gather_1, i + 1, other)
        stage(down_peer, i - 1)
        stage(scatter_5, i - 3)
        return carry

    gather_1_first()
    unpack(0, pieces // 2)
    lax.fori_loop(0, groups + 3, turn, 0)
    wait_send(part.at[co], pds.at[groups - 1])
    wait_send(part.at[c, pl.ds(0, 3)], rsend.at[groups - 1])
    for g in range(groups):
        wait_send(zin.at[g], zsend.at[g])


def on_device(section_out, expert_ids, gate_weights, w_gate_up, w_down):
    rows, width = section_out.shape[1:]
    units = w_down.shape[2]
    groups = rows // ROWS
    quarter = width // 4
    hbm = pl.BlockSpec(memory_space=pl.ANY)
    vmem = pl.BlockSpec(memory_space=pltpu.VMEM)
    dma = pltpu.SemaphoreType.DMA
    regular = pltpu.SemaphoreType.REGULAR
    result = pl.pallas_call(
        moe_kernel,
        out_shape=jax.ShapeDtypeStruct((rows, width), BF),
        in_specs=[hbm, vmem, vmem, hbm, hbm],
        out_specs=vmem,
        scratch_shapes=[
            pltpu.VMEM((2, 2, 4, 4, ROWS, EXT + width), BF),
            pltpu.VMEM((groups, ROWS, width), BF),
            pltpu.VMEM((ROWS, width), BF),
            pltpu.VMEM((groups, ROWS, EXT), BF),
            pltpu.VMEM((2, width // 8, 2, units), BF),
            pltpu.VMEM((width, 2 * units), BF),
            pltpu.VMEM((units, width), BF),
            pltpu.VMEM((32 * ROWS, 2 * units), F32),
            pltpu.VMEM((32 * ROWS, units), BF),
            pltpu.VMEM((2, 4, 4, ROWS, width), BF),
            pltpu.VMEM((4, 4, ROWS, width), BF),
            pltpu.VMEM((groups, 4, 3, 4, ROWS, quarter), BF),
            pltpu.VMEM((4, 4, ROWS, quarter), BF),
            pltpu.VMEM((groups, 4, 3, ROWS, quarter), BF),
            dma((4,)), dma((groups,)), dma((groups + 1,)),
            dma((groups, 17)), dma((groups, 5)),
            dma((groups, 4)), dma((groups,)),
            dma((groups, 4)), dma((groups, 4)), dma((groups, 4, 4)), dma((groups,)),
            dma((groups, 4)), dma((groups, 4)), dma((groups,)),
            regular((groups,)), regular((groups,)),
        ],
        compiler_params=pltpu.CompilerParams(
            collective_id=0, has_side_effects=True, vmem_limit_bytes=58_500_000
        ),
        name="moe",
    )(section_out[0], expert_ids[0].T, gate_weights[0].T, w_gate_up[0, 0], w_down[0, 0])
    return result[None]


def solution(mesh):
    return jax.shard_map(
        on_device,
        mesh=mesh,
        in_specs=(
            P("section", ("ex", "ey"), None),
            P("section", ("ex", "ey"), None),
            P("section", ("ex", "ey"), None),
            P("section", "ey", None, None, "ex"),
            P("section", "ey", "ex", None),
        ),
        out_specs=P("section", ("ex", "ey"), None),
        check_vma=False,
    )
```
